256 devices in a mesh: wide: 32 (over z, y_lo, core), narrow: 8 (over x, y_hi).
Axes of the slice: x: 4, y: 4 (y_hi: 2, y_lo: 2; y = y_hi * 2 + y_lo), z: 8, core: 2. Of those that a mesh axis runs over, the one named last changes fastest.
Arguments:
- left: bfloat16 [64, 2048, 1024], P(None, 'wide', 'narrow'), may hold values from -6 to 6
- right: bfloat16 [64, 2048, 1024], P(None, 'wide', 'narrow'), may hold values from -6 to 6
- bond_signs: int32 [4, 8, 2048, 1024], P(None, None, 'wide', 'narrow'), may hold values from 0 to 1
- hop: float32 [4, 4], replicated, may hold values from 0.2 to 1
Outputs:
- moments: float32 [16, 64, 64], P(None, 'wide', 'narrow')
The draws below stay inside these ranges and needn't reach their ends.
All inputs are finite; a program needn't handle non-finite values.
Results may differ from the reference program's by a relative error of at most 0.004.
Values may be sent and summed in bfloat16 or wider, within the bound.
A program may use at most 64 MiB of HBM per device.

```python
import math
import jax
import jax.numpy as jnp
from jax import lax

NL = 64
NR = 64
OPS = 4
RANGE = 4
NX = 2048
NY = 1024


def touch_ends(drawn, rng, least, high):
    spot = [jax.random.randint(jax.random.fold_in(rng, axis), (), 0, length) for axis, length in enumerate(drawn.shape)]
    main_axis = drawn.shape.index(max(drawn.shape))
    beside = spot[:main_axis] + [(spot[main_axis] + 1) % drawn.shape[main_axis]] + spot[main_axis + 1:]
    return drawn.at[tuple(spot)].set(least).at[tuple(beside)].set(high)


def block_levels(rng, shape, pieces, low, high):
    level, own = 1.0, jax.random.fold_in(rng, 6)
    for position, parts in pieces:
        heights = jnp.exp(jax.random.uniform(jax.random.fold_in(own, position), (parts,), jnp.float32, low / len(pieces), high / len(pieces)))
        level = level * jnp.repeat(heights, shape[position] // parts).reshape([-1 if axis == position else 1 for axis in range(len(shape))])
    return level


def gaussian(key, extent, deviation, limit, split=(), kind=jnp.bfloat16):
    loudness = block_levels(key, extent, split, -0.22, 0.18) if split else 1.0
    drawn = jax.random.normal(key, extent, jnp.float32) * deviation * loudness
    return jnp.minimum(jnp.maximum(drawn, -limit), limit).astype(kind)


def setup_inputs(seed: int = 0) -> dict:
    seeds = jax.random.split(jax.random.key(seed), 5)
    left = gaussian(seeds[0], (NL, NX, NY), 1.0, 6.0, ((1, 32), (2, 8)))
    right = gaussian(seeds[1], (NR, NX, NY), 1.0, 6.0, ((1, 32), (2, 8)))
    bond_signs = touch_ends(jax.random.randint(seeds[2], (OPS, 2 * RANGE, NX, NY), 0, 2), jax.random.fold_in(seeds[2], 1), 0, 1).astype(jnp.int32)
    hop = jnp.clip(jnp.exp(jax.random.uniform(seeds[3], (OPS, RANGE), jnp.float32, math.log(0.2), math.log(1.0))), 0.2, 1.0)
    return dict(left=left, right=right, bond_signs=bond_signs, hop=hop)


def current_full(vectors, sign_bits, coefficient, direction):
    signs_float = (2 * sign_bits - 1).astype(jnp.float32)
    summed = jnp.zeros(vectors.shape, jnp.float32)
    for index in range(RANGE):
        offset = index + 1
        ahead = jnp.roll(vectors, -offset, axis=direction).astype(jnp.float32)
        behind = jnp.roll(vectors, offset, axis=direction).astype(jnp.float32)
        summed = summed + coefficient[index] * (signs_float[index] * ahead - signs_float[RANGE + index] * behind)
    return summed

def adjoint_full(vectors, sign_bits, coefficient, direction):
    signs_float = (2 * sign_bits - 1).astype(jnp.float32)
    values = vectors.astype(jnp.float32)
    summed = jnp.zeros(vectors.shape, jnp.float32)
    for index in range(RANGE):
        offset = index + 1
        forward = jnp.roll(signs_float[index] * values, offset, axis=direction)
        backward = jnp.roll(signs_float[RANGE + index] * values, -offset, axis=direction)
        summed = summed + coefficient[index] * (forward - backward)
    return summed

def reference(left, right, bond_signs, hop):
    left_blocks = left.reshape(NL // 8, 8, NX, NY)
    right_blocks = right.reshape(NR // 8, 8, NX, NY)

    def right_block(block_right):
        first = jnp.stack([current_full(block_right, bond_signs[inner], hop[inner], 1 + inner % 2).astype(jnp.bfloat16) for inner in range(OPS)]).reshape(OPS * 8, NX * NY)

        def left_block(block_left):
            back = jnp.stack([adjoint_full(block_left, bond_signs[outer], hop[outer], 1 + outer % 2).astype(jnp.bfloat16) for outer in range(OPS)]).reshape(OPS * 8, NX * NY)
            return jnp.dot(back, first.T, preferred_element_type=jnp.float32)
        return lax.map(left_block, left_blocks)
    mapped = lax.map(right_block, right_blocks).reshape(NR // 8, NL // 8, OPS, 8, OPS, 8)
    moments = jnp.transpose(mapped, (2, 4, 1, 3, 0, 5)).reshape(OPS * OPS, NL, NR)
    return moments * jnp.float32(1.0 / math.sqrt(NX * NY))
```

```python
import functools
import math

import jax
import jax.numpy as jnp
from jax import lax
from jax.experimental import pallas as pl
from jax.experimental.pallas import tpu as pltpu
from jax.sharding import PartitionSpec as P

OPS = 4
RANGE = 4
VECS = 64
ROWS = 64
COLS = 128
PITCH = 72
MESH = pl.DeviceIdType.MESH
F32 = jnp.float32
BF16 = jnp.bfloat16


def stencil_kernel(
    scale, left_ref, right_ref, bits_ref, hop_ref, out_ref,
    flat, field_r, field_l, weight, weight_adj, packed, first, product,
    row_send, row_recv, col_send, col_recv, sr_stage, sr_send, sr_recv, sc_send, sc_recv,
    send_sem, recv_sem,
):
    wide_size = lax.axis_size("wide")
    narrow_size = lax.axis_size("narrow")
    wide = lax.axis_index("wide")
    narrow = lax.axis_index("narrow")
    w_up, w_down = lax.rem(wide + 1, wide_size), lax.rem(wide + wide_size - 1, wide_size)
    n_up, n_down = lax.rem(narrow + 1, narrow_size), lax.rem(narrow + narrow_size - 1, narrow_size)
    sides = ((w_up, narrow), (w_down, narrow), (wide, n_up), (wide, n_down))

    barrier = pltpu.get_barrier_semaphore()
    for device in sides:
        pl.semaphore_signal(barrier, inc=1, device_id=device, device_id_type=MESH)

    lane = lax.broadcasted_iota(jnp.int32, (VECS, COLS), 1)

    def transposed(source, field):
        @pl.loop(0, VECS)
        def _(v):
            flat[pl.ds(pl.multiple_of(v * PITCH, 8), ROWS), :] = source[v].astype(F32)

        @pl.loop(0, ROWS)
        def _(row):
            for g in range(VECS // 8):
                field[row + RANGE, 8 * g : 8 * g + 8, :] = flat[
                    pl.ds(8 * g * PITCH + row, 8, stride=PITCH), :
                ]

    def edges(side, field):
        row_send[side, 0] = field[ROWS : ROWS + RANGE].astype(BF16)
        row_send[side, 1] = field[RANGE : 2 * RANGE].astype(BF16)

        def pack(i, held):
            held = list(held)
            inside = lax.shift_right_logical(lane, 2) == i
            for half in range(2):
                x = field[RANGE + 32 * half + i]
                up = pltpu.roll(x, lax.rem(4 * i + 4, COLS), 1)
                down = pltpu.roll(x, 4 * i, 1)
                held[half] = jnp.where(inside, up, held[half])
                held[2 + half] = jnp.where(inside, down, held[2 + half])
            return tuple(held)

        zero = jnp.zeros((VECS, COLS), F32)
        held = lax.fori_loop(0, 32, pack, (zero,) * 4)
        for half in range(2):
            col_send[side, 0, half] = held[half].astype(BF16)
            col_send[side, 1, half] = held[2 + half].astype(BF16)

    def copies(slot, row_pair, col_pair):
        made = []
        for way in range(4):
            (source, target), part = (row_pair, way) if way < 2 else (col_pair, way - 2)
            made.append(
                pltpu.make_async_remote_copy(
                    src_ref=source.at[part],
                    dst_ref=target.at[part],
                    send_sem=send_sem.at[slot, way],
                    recv_sem=recv_sem.at[slot, way],
                    device_id=sides[way],
                    device_id_type=MESH,
                )
            )
        return made

    def landed(side, field, moves):
        for move in moves:
            move.wait_recv()
        field[0:RANGE] = row_recv[side, 0].astype(F32)
        field[ROWS + RANGE : ROWS + 2 * RANGE] = row_recv[side, 1].astype(F32)
        for half in range(2):
            packed[0, half] = col_recv[side, 0, half].astype(F32)
            packed[1, half] = col_recv[side, 1, half].astype(F32)

    transposed(right_ref, field_r)
    edges(0, field_r)
    pl.semaphore_wait(barrier, 4)
    moves_r = copies(0, (row_send.at[0], row_recv.at[0]), (col_send.at[0], col_recv.at[0]))
    for move in moves_r:
        move.start()

    def coefficient(op, tap):
        return hop_ref[op, tap % RANGE] * (1.0 if tap < RANGE else -1.0)

    small = lax.broadcasted_iota(jnp.int32, (ROWS, COLS), 1)
    for half, op in enumerate((0, 2)):
        for tap in range(2 * RANGE):
            sign = (2 * bits_ref[op, tap] - 1).astype(F32)
            weight[8 * op + tap, 8 : 8 + ROWS, :] = coefficient(op, tap) * sign
            way, at = (0, ROWS - RANGE) if tap < RANGE else (1, 0)
            spot = (4 * half + tap % RANGE) * RANGE
            sr_stage[way, spot : spot + RANGE, :] = sign[at : at + RANGE]
    for way in range(2):
        sr_send[way] = sr_stage[way].astype(BF16)
    for way in range(2):
        held = jnp.zeros((ROWS, COLS), F32)
        for half, op in enumerate((1, 3)):
            for k in range(RANGE):
                tap = RANGE * way + k
                spot = 4 * half + k
                sign = (2 * bits_ref[op, tap] - 1).astype(F32)
                weight[8 * op + tap, 8 : 8 + ROWS, :] = coefficient(op, tap) * sign
                moved = pltpu.roll(sign, 4 * spot + 4 if way == 0 else 4 * spot, 1)
                held = jnp.where(lax.shift_right_logical(small, 2) == spot, moved, held)
        sc_send[way] = held.astype(BF16)

    transposed(left_ref, field_l)
    edges(1, field_l)
    moves_l = copies(1, (row_send.at[1], row_recv.at[1]), (col_send.at[1], col_recv.at[1]))
    moves_s = copies(2, (sr_send, sr_recv), (sc_send, sc_recv))
    for move in moves_l + moves_s:
        move.start()

    def along_rows(field, row, adjoint):
        sums = [None, None]
        for tap in range(2 * RANGE):
            k = tap % RANGE + 1
            step = k if tap < RANGE else -k
            step = -step if adjoint else step
            x = field[RANGE + row + step]
            for half, op in enumerate((0, 2)):
                at = 8 + row + (step if adjoint else 0)
                term = weight[8 * op + tap, pl.ds(at, 1), :] * x
                sums[half] = term if sums[half] is None else sums[half] + term
        return sums

    def along_cols(field, row, adjoint):
        x = field[RANGE + row]
        half = row // 32
        spot = 4 * (row % 32)
        low = pltpu.roll(packed[0, half], lax.rem(2 * COLS - 4 - spot, COLS), 1)
        high = pltpu.roll(packed[1, half], lax.rem(COLS - spot, COLS), 1)
        halo = jnp.where(lane < COLS // 2, high, low)
        sums = [None, None]
        for tap in range(2 * RANGE):
            k = tap % RANGE + 1
            ahead = (tap < RANGE) != adjoint
            if ahead:
                moved = pltpu.roll(jnp.where(lane < k, halo, x), COLS - k, 1)
            else:
                moved = pltpu.roll(jnp.where(lane >= COLS - k, halo, x), k, 1)
            for half_op, op in enumerate((1, 3)):
                if adjoint:
                    w = weight_adj[8 * half_op + tap, pl.ds(row, 1), :]
                else:
                    w = weight[8 * op + tap, pl.ds(8 + row, 1), :]
                term = w * moved
                sums[half_op] = term if sums[half_op] is None else sums[half_op] + term
        return sums

    for move in moves_r:
        move.wait_send()
    landed(0, field_r, moves_r)

    @pl.loop(0, ROWS // 2)
    def _(pair):
        for j in range(2):
            sums = along_rows(field_r, 2 * pair + j, False)
            for half, op in enumerate((0, 2)):
                first[pair, VECS * op : VECS * (op + 1), COLS * j : COLS * (j + 1)] = sums[half].astype(BF16)

    @pl.loop(0, ROWS // 2)
    def _(pair):
        for j in range(2):
            sums = along_cols(field_r, 2 * pair + j, False)
            for half, op in enumerate((1, 3)):
                first[pair, VECS * op : VECS * (op + 1), COLS * j : COLS * (j + 1)] = sums[half].astype(BF16)

    for move in moves_l + moves_s:
        move.wait_send()
    for move in moves_s:
        move.wait_recv()
    landed(1, field_l, moves_l)

    for way in range(2):
        sr_stage[way] = sr_recv[way].astype(F32)
    for half, op in enumerate((0, 2)):
        for tap in range(2 * RANGE):
            way, at = (0, 8 - RANGE) if tap < RANGE else (1, 8 + ROWS)
            spot = (4 * half + tap % RANGE) * RANGE
            weight[8 * op + tap, at : at + RANGE, :] = coefficient(op, tap) * sr_stage[way, spot : spot + RANGE, :]
    for way in range(2):
        halo_signs = sc_recv[way].astype(F32)
        for half, op in enumerate((1, 3)):
            for tap in range(RANGE * way, RANGE * way + RANGE):
                k = tap % RANGE + 1
                spot = 4 * half + tap % RANGE
                own = weight[8 * op + tap, 8 : 8 + ROWS, :]
                if way == 0:
                    halo = coefficient(op, tap) * pltpu.roll(halo_signs, (COLS - 4 - 4 * spot) % COLS, 1)
                    moved = pltpu.roll(jnp.where(small >= COLS - k, halo, own), k, 1)
                else:
                    halo = coefficient(op, tap) * pltpu.roll(halo_signs, (COLS - 4 * spot) % COLS, 1)
                    moved = pltpu.roll(jnp.where(small < k, halo, own), COLS - k, 1)
                weight_adj[8 * half + tap] = moved

    product[...] = jnp.zeros_like(product)

    def gram(pair, along, ops):
        halves = [along(field_l, 2 * pair + j, True) for j in range(2)]
        back = jnp.concatenate(
            [
                jnp.concatenate([halves[j][half].astype(BF16) for j in range(2)], axis=1)
                for half in range(2)
            ],
            axis=0,
        )
        part = lax.dot_general(back, first[pair], (((1,), (1,)), ((), ())), preferred_element_type=F32)
        for half, op in enumerate(ops):
            for h in range(2):
                product[h, VECS * op : VECS * (op + 1), :] += part[
                    VECS * half : VECS * (half + 1), COLS * h : COLS * (h + 1)
                ]

    @pl.loop(0, ROWS // 2)
    def _(pair):
        gram(pair, along_rows, (0, 2))

    @pl.loop(0, ROWS // 2)
    def _(pair):
        gram(pair, along_cols, (1, 3))

    @pl.loop(0, VECS // 2)
    def _(block):
        for h in range(2):
            for i in range(2):
                out_ref[block % 2, block // 2, 4 * i : 4 * i + 4, COLS * h : COLS * (h + 1)] = scale * product[
                    h, pl.ds(2 * block + i, 4, stride=VECS), :
                ]


def sum_kernel(
    chips, part_ref, out_ref, own, arrived_core, arrived_wide, whole, arrived_narrow,
    core_send, core_recv, wide_send, wide_recv, narrow_send, narrow_recv,
):
    narrow_size = lax.axis_size("narrow")
    wide = lax.axis_index("wide")
    narrow = lax.axis_index("narrow")
    core, chip = lax.rem(wide, 2), wide // 2
    partner = (wide + 1 - 2 * core, narrow)
    in_wide = [(2 * lax.rem(chip + d, chips) + core, narrow) for d in range(1, chips)]
    in_narrow = [(wide, lax.rem(narrow + d, narrow_size)) for d in range(1, narrow_size)]

    barrier = pltpu.get_barrier_semaphore()
    everyone = [partner] + in_wide + in_narrow
    for device in everyone:
        pl.semaphore_signal(barrier, inc=1, device_id=device, device_id_type=MESH)
    pl.semaphore_wait(barrier, len(everyone))

    def remote(source, target, sent, received, device):
        return pltpu.make_async_remote_copy(
            src_ref=source, dst_ref=target, send_sem=sent, recv_sem=received,
            device_id=device, device_id_type=MESH,
        )

    swap = remote(part_ref.at[1 - core], arrived_core, core_send.at[0], core_recv.at[0], partner)
    swap.start()
    swap.wait()
    own[...] = part_ref[core] + arrived_core[...]

    moves = []
    for d, device in enumerate(in_wide):
        target = lax.rem(chip + d + 1, chips)
        moves.append(remote(own.at[target], arrived_wide.at[d], wide_send.at[d], wide_recv.at[d], device))
    for move in moves:
        move.start()
    for move in moves:
        move.wait_recv()
    total = own[chip]
    for d in range(chips - 1):
        total = total + arrived_wide[d]
    whole[...] = total
    for move in moves:
        move.wait_send()

    moves = []
    for d, device in enumerate(in_narrow):
        moves.append(remote(whole, arrived_narrow.at[d], narrow_send.at[d], narrow_recv.at[d], device))
    for move in moves:
        move.start()
    for move in moves:
        move.wait_recv()
    total = whole[...]
    for d in range(narrow_size - 1):
        total = total + arrived_narrow[d]
    turn = lax.rem(COLS - 8 * narrow, COLS)
    for h in range(2):
        out_ref[:, COLS * h : COLS * (h + 1)] = pltpu.roll(total[:, COLS * h : COLS * (h + 1)], turn, 1)
    for move in moves:
        move.wait_send()


def on_device(left, right, bond_signs, hop):
    wide_size = lax.axis_size("wide")
    narrow_size = lax.axis_size("narrow")
    chips = wide_size // 2
    scale = 1.0 / math.sqrt(ROWS * COLS * wide_size * narrow_size)
    vmem = pl.BlockSpec(memory_space=pltpu.VMEM)
    smem = pl.BlockSpec(memory_space=pltpu.SMEM)
    part = pl.pallas_call(
        functools.partial(stencil_kernel, scale),
        out_shape=jax.ShapeDtypeStruct((2, chips, 8, OPS * VECS), F32),
        in_specs=[vmem, vmem, vmem, smem],
        out_specs=vmem,
        scratch_shapes=[
            pltpu.VMEM((VECS * PITCH, COLS), F32),
            pltpu.VMEM((ROWS + 2 * RANGE, VECS, COLS), F32),
            pltpu.VMEM((ROWS + 2 * RANGE, VECS, COLS), F32),
            pltpu.VMEM((8 * OPS, ROWS + 16, COLS), F32),
            pltpu.VMEM((16, ROWS, COLS), F32),
            pltpu.VMEM((2, 2, VECS, COLS), F32),
            pltpu.VMEM((ROWS // 2, OPS * VECS, 2 * COLS), BF16),
            pltpu.VMEM((2, OPS * VECS, COLS), F32),
            pltpu.VMEM((2, 2, RANGE, VECS, COLS), BF16),
            pltpu.VMEM((2, 2, RANGE, VECS, COLS), BF16),
            pltpu.VMEM((2, 2, 2, VECS, COLS), BF16),
            pltpu.VMEM((2, 2, 2, VECS, COLS), BF16),
            pltpu.VMEM((2, 8 * RANGE, COLS), F32),
            pltpu.VMEM((2, 8 * RANGE, COLS), BF16),
            pltpu.VMEM((2, 8 * RANGE, COLS), BF16),
            pltpu.VMEM((2, ROWS, COLS), BF16),
            pltpu.VMEM((2, ROWS, COLS), BF16),
            pltpu.SemaphoreType.DMA((3, 4)),
            pltpu.SemaphoreType.DMA((3, 4)),
        ],
        compiler_params=pltpu.CompilerParams(
            collective_id=0, has_side_effects=True, vmem_limit_bytes=48 << 20
        ),
        name="stencil",
    )(left, right, bond_signs, hop)
    spread = pl.pallas_call(
        functools.partial(sum_kernel, chips),
        out_shape=jax.ShapeDtypeStruct((8, OPS * VECS), F32),
        in_specs=[vmem],
        out_specs=vmem,
        scratch_shapes=[
            pltpu.VMEM((chips, 8, OPS * VECS), F32),
            pltpu.VMEM((chips, 8, OPS * VECS), F32),
            pltpu.VMEM((chips - 1, 8, OPS * VECS), F32),
            pltpu.VMEM((8, OPS * VECS), F32),
            pltpu.VMEM((narrow_size - 1, 8, OPS * VECS), F32),
            pltpu.SemaphoreType.DMA((1,)),
            pltpu.SemaphoreType.DMA((1,)),
            pltpu.SemaphoreType.DMA((chips - 1,)),
            pltpu.SemaphoreType.DMA((chips - 1,)),
            pltpu.SemaphoreType.DMA((narrow_size - 1,)),
            pltpu.SemaphoreType.DMA((narrow_size - 1,)),
        ],
        compiler_params=pltpu.CompilerParams(collective_id=1, has_side_effects=True),
        name="spread_sum",
    )(part)
    wanted = spread.reshape(2, OPS, OPS, VECS)[..., : VECS // narrow_size]
    return wanted.transpose(1, 2, 0, 3).reshape(OPS * OPS, 2, VECS // narrow_size)


def solution(mesh):
    in_specs = (
        P(None, "wide", "narrow"),
        P(None, "wide", "narrow"),
        P(None, None, "wide", "narrow"),
        P(),
    )
    return jax.shard_map(
        on_device, mesh=mesh, in_specs=in_specs, out_specs=P(None, "wide", "narrow"), check_vma=False
    )
```

```python
import functools
import math

import jax
import jax.numpy as jnp
from jax import lax
from jax.experimental import pallas as pl
from jax.experimental.pallas import tpu as pltpu
from jax.sharding import PartitionSpec as P

OPS = 4
RANGE = 4
VECS = 64
ROWS = 64
COLS = 128
PITCH = 72
BANDS = ROWS // RANGE
STEPS = (1, 2, 3, 4, -1, -2, -3, -4)
MESH = pl.DeviceIdType.MESH
F32 = jnp.float32
BF16 = jnp.bfloat16


def iota(shape, dim):
    return lax.broadcasted_iota(jnp.int32, shape, dim)


def ones_where(condition):
    return jnp.where(condition, 1.0, 0.0).astype(BF16)


def moments_kernel(
    scale, chips, left_hbm, right_hbm, bits_hbm, hop_hbm, out_ref,
    left_ref, right_ref, bits_ref, hop_ref,
    flat, field_r, field_l, plain_r, plain_l, weight, weight_adj, shifter, packed_r, packed_l,
    first, product,
    row_send, row_recv, col_send, col_recv, sr_stage, sr_send, sr_recv, sc_send, sc_recv,
    parts, own, arrived_core, arrived_wide, whole, arrived_narrow,
    load_sem, send_sem, recv_sem, core_send, core_recv, wide_send, wide_recv, narrow_send, narrow_recv,
):
    loads = [
        pltpu.make_async_copy(source, target, load_sem.at[i])
        for i, (source, target) in enumerate(
            ((right_hbm, right_ref), (bits_hbm, bits_ref), (hop_hbm, hop_ref), (left_hbm, left_ref))
        )
    ]
    for load in loads:
        load.start()

    wide_size = lax.axis_size("wide")
    narrow_size = lax.axis_size("narrow")
    wide = lax.axis_index("wide")
    narrow = lax.axis_index("narrow")
    w_up, w_down = lax.rem(wide + 1, wide_size), lax.rem(wide + wide_size - 1, wide_size)
    n_up, n_down = lax.rem(narrow + 1, narrow_size), lax.rem(narrow + narrow_size - 1, narrow_size)
    sides = ((w_up, narrow), (w_down, narrow), (wide, n_up), (wide, n_down))
    core, chip = lax.rem(wide, 2), wide // 2
    partner = (wide + 1 - 2 * core, narrow)
    in_wide = [(2 * lax.rem(chip + d, chips) + core, narrow) for d in range(1, chips)]
    in_narrow = [(wide, lax.rem(narrow + d, narrow_size)) for d in range(1, narrow_size)]

    barrier = pltpu.get_barrier_semaphore()
    everyone = [sides[0], sides[1]] + in_wide + in_narrow
    for device in everyone:
        pl.semaphore_signal(barrier, inc=1, device_id=device, device_id_type=MESH)

    def remote(source, target, sent, received, device):
        return pltpu.make_async_remote_copy(
            src_ref=source, dst_ref=target, send_sem=sent, recv_sem=received,
            device_id=device, device_id_type=MESH,
        )

    kappa = iota((2 * COLS, COLS), 0)
    tail = kappa - COLS
    edge = jnp.where(tail < COLS // 2, tail % RANGE - RANGE, tail % RANGE + COLS)
    origin = jnp.where(kappa < COLS, kappa, edge) - iota((2 * COLS, COLS), 1)
    for t, step in enumerate(STEPS):
        shifter[:, COLS * t : COLS * (t + 1)] = ones_where(origin == step)

    spot_row = iota((COLS, 2 * COLS), 0)
    spot_band = spot_row % (COLS // 2) // RANGE
    spot_col = spot_row % RANGE + jnp.where(spot_row < COLS // 2, COLS - RANGE, 0)
    spot_lane = COLS * spot_band + spot_col - iota((COLS, 2 * COLS), 1)

    def transposed(source, field, plain):
        @pl.loop(0, VECS)
        def _(v):
            flat[pl.ds(pl.multiple_of(v * PITCH, 8), ROWS), :] = source[v].astype(F32)

        @pl.loop(0, ROWS)
        def _(row):
            groups = [flat[pl.ds(8 * g * PITCH + row, 8, stride=PITCH), :] for g in range(VECS // 8)]
            whole_row = jnp.concatenate(groups, axis=0)
            field[row + RANGE] = whole_row
            plain[row] = whole_row.astype(BF16)

    def edges(side, plain):
        row_send[side, 0] = plain[ROWS - RANGE : ROWS]
        row_send[side, 1] = plain[0:RANGE]
        picked = jnp.zeros((COLS, 2 * COLS), F32)
        for c in range(BANDS // 2):
            pick = ones_where(spot_lane == 2 * COLS * c)
            bands = [
                plain[RANGE * b : RANGE * (b + 1)].reshape(RANGE * VECS, COLS)
                for b in (2 * c, 2 * c + 1)
            ]
            picked = picked + lax.dot_general(
                pick, jnp.concatenate(bands, axis=1), (((1,), (1,)), ((), ())),
                preferred_element_type=F32,
            )
        col_send[side, 0] = picked[: COLS // 2].astype(BF16)
        col_send[side, 1] = picked[COLS // 2 :].astype(BF16)

    def copies(slot, row_pair, col_pair):
        made = []
        for way in range(4):
            (source, target), part = (row_pair, way) if way < 2 else (col_pair, way - 2)
            made.append(
                remote(
                    source.at[part], target.at[part], send_sem.at[slot, way], recv_sem.at[slot, way],
                    sides[way],
                )
            )
        return made

    def landed(side, field, packed, moves):
        for move in moves:
            move.wait_recv()
        field[0:RANGE] = row_recv[side, 0].astype(F32)
        field[ROWS + RANGE : ROWS + 2 * RANGE] = row_recv[side, 1].astype(F32)
        strips = jnp.concatenate([col_recv[side, way].astype(F32) for way in range(2)], axis=0)
        packed[...] = jnp.transpose(strips).astype(BF16).reshape(RANGE, VECS, COLS)

    loads[0].wait()
    transposed(right_ref, field_r, plain_r)
    edges(0, plain_r)
    pl.semaphore_wait(barrier, len(everyone))
    moves_r = copies(0, (row_send.at[0], row_recv.at[0]), (col_send.at[0], col_recv.at[0]))
    for move in moves_r:
        move.start()

    loads[3].wait()
    transposed(left_ref, field_l, plain_l)
    edges(1, plain_l)
    moves_l = copies(1, (row_send.at[1], row_recv.at[1]), (col_send.at[1], col_recv.at[1]))
    for move in moves_l:
        move.start()

    loads[1].wait()
    loads[2].wait()

    def coefficient(op, tap):
        return hop_ref[op, tap % RANGE] * (1.0 if tap < RANGE else -1.0)

    def sign_of(op, tap):
        return (2 * bits_ref[op, tap] - 1).astype(F32)

    small = iota((ROWS, COLS), 1)
    for half, op in enumerate((0, 2)):
        for tap in range(2 * RANGE):
            sign = sign_of(op, tap)
            weight[8 * op + tap, 8 : 8 + ROWS, :] = coefficient(op, tap) * sign
            way, at = (0, ROWS - RANGE) if tap < RANGE else (1, 0)
            spot = (4 * half + tap % RANGE) * RANGE
            sr_stage[way, spot : spot + RANGE, :] = sign[at : at + RANGE]
    for way in range(2):
        sr_send[way] = sr_stage[way].astype(BF16)
    for way in range(2):
        held = jnp.zeros((ROWS, COLS), F32)
        for half, op in enumerate((1, 3)):
            for k in range(RANGE):
                tap = RANGE * way + k
                sign = sign_of(op, tap)
                weight[8 * op + tap, 8 : 8 + ROWS, :] = coefficient(op, tap) * sign
                at = COLS // 2 * way + RANGE * (4 * half + k)
                moved = pltpu.roll(sign, at + RANGE if way == 0 else at, 1) if at or way == 0 else sign
                held = jnp.where(small // RANGE == at // RANGE, moved, held)
        sc_send[way] = held.astype(BF16)
    moves_s = copies(2, (sr_send, sr_recv), (sc_send, sc_recv))
    for move in moves_s:
        move.start()

    def along_rows(field, row, adjoint):
        sums = [None, None]
        for tap in range(2 * RANGE):
            step = -STEPS[tap] if adjoint else STEPS[tap]
            x = field[RANGE + row + step]
            for half, op in enumerate((0, 2)):
                at = 8 + row + (step if adjoint else 0)
                term = weight[8 * op + tap, pl.ds(at, 1), :] * x
                sums[half] = term if sums[half] is None else sums[half] + term
        return sums

    wide_lane = iota((VECS, COLS), 1) % (COLS // 2) // RANGE

    def along_cols(plain, packed, pair, adjoint):
        band = pair // 2
        inside = wide_lane == band
        rows = []
        for j in range(2):
            strip = packed[2 * lax.rem(pair, 2) + j]
            rows.append(
                jnp.concatenate([plain[2 * pair + j], jnp.where(inside, strip, jnp.zeros_like(strip))], axis=1)
            )
        lhs = jnp.concatenate(rows, axis=0)
        sums = [[None, None], [None, None]]
        for t in range(0, 2 * RANGE, 2):
            moved = jnp.dot(lhs, shifter[:, COLS * t : COLS * (t + 2)], preferred_element_type=F32)
            for u in range(2):
                tap = (t + u + RANGE) % (2 * RANGE) if adjoint else t + u
                for j in range(2):
                    x = moved[VECS * j : VECS * (j + 1), COLS * u : COLS * (u + 1)]
                    for half, op in enumerate((1, 3)):
                        if adjoint:
                            w = weight_adj[8 * half + tap, pl.ds(2 * pair + j, 1), :]
                        else:
                            w = weight[8 * op + tap, pl.ds(8 + 2 * pair + j, 1), :]
                        term = w * x
                        sums[j][half] = term if sums[j][half] is None else sums[j][half] + term
        return sums

    def applied(field, plain, packed, pair, adjoint):
        cols = along_cols(plain, packed, pair, adjoint)
        rows = [along_rows(field, 2 * pair + j, adjoint) for j in range(2)]
        by_op = []
        for op in range(OPS):
            source = cols if op % 2 else rows
            by_op.append(
                jnp.concatenate([source[j][op // 2].astype(BF16) for j in range(2)], axis=1)
            )
        return jnp.concatenate(by_op, axis=0)

    for move in moves_r:
        move.wait_send()
    landed(0, field_r, packed_r, moves_r)

    @pl.loop(0, ROWS // 2)
    def _(pair):
        first[pair] = applied(field_r, plain_r, packed_r, pair, False)

    for move in moves_l + moves_s:
        move.wait_send()
    for move in moves_s:
        move.wait_recv()
    landed(1, field_l, packed_l, moves_l)

    for way in range(2):
        sr_stage[way] = sr_recv[way].astype(F32)
    for half, op in enumerate((0, 2)):
        for tap in range(2 * RANGE):
            way, at = (0, 8 - RANGE) if tap < RANGE else (1, 8 + ROWS)
            spot = (4 * half + tap % RANGE) * RANGE
            weight[8 * op + tap, at : at + RANGE, :] = coefficient(op, tap) * sr_stage[way, spot : spot + RANGE, :]
    strips = sc_recv[0].astype(F32) + sc_recv[1].astype(F32)
    for tap in range(2 * RANGE):
        lhs = []
        for half, op in enumerate((1, 3)):
            spot = 4 * half + tap % RANGE
            inside = small % (COLS // 2) // RANGE == spot
            lhs.append(jnp.concatenate([sign_of(op, tap), jnp.where(inside, strips, 0.0)], axis=1))
        t = (tap + RANGE) % (2 * RANGE)
        moved = jnp.dot(
            jnp.concatenate(lhs, axis=0).astype(BF16), shifter[:, COLS * t : COLS * (t + 1)],
            preferred_element_type=F32,
        )
        for half, op in enumerate((1, 3)):
            weight_adj[8 * half + tap] = coefficient(op, tap) * moved[ROWS * half : ROWS * (half + 1)]

    product[...] = jnp.zeros_like(product)

    @pl.loop(0, ROWS // 2)
    def _(pair):
        back = applied(field_l, plain_l, packed_l, pair, True)
        part = lax.dot_general(back, first[pair], (((1,), (1,)), ((), ())), preferred_element_type=F32)
        for h in range(2):
            product[h] += part[:, COLS * h : COLS * (h + 1)]

    @pl.loop(0, VECS // 2)
    def _(block):
        for h in range(2):
            for i in range(2):
                parts[block % 2, block // 2, 4 * i : 4 * i + 4, COLS * h : COLS * (h + 1)] = scale * product[
                    h, pl.ds(2 * block + i, 4, stride=VECS), :
                ]

    swap = remote(parts.at[1 - core], arrived_core, core_send.at[0], core_recv.at[0], partner)
    swap.start()
    swap.wait()
    own[...] = parts[core] + arrived_core[...]

    moves = []
    for d, device in enumerate(in_wide):
        target = lax.rem(chip + d + 1, chips)
        moves.append(remote(own.at[target], arrived_wide.at[d], wide_send.at[d], wide_recv.at[d], device))
    for move in moves:
        move.start()
    for move in moves:
        move.wait_recv()
    total = own[chip]
    for d in range(chips - 1):
        total = total + arrived_wide[d]
    whole[...] = total
    for move in moves:
        move.wait_send()

    moves = []
    for d, device in enumerate(in_narrow):
        moves.append(remote(whole, arrived_narrow.at[d], narrow_send.at[d], narrow_recv.at[d], device))
    for move in moves:
        move.start()
    for move in moves:
        move.wait_recv()
    total = whole[...]
    for d in range(narrow_size - 1):
        total = total + arrived_narrow[d]
    turn = lax.rem(COLS - 8 * narrow, COLS)
    for h in range(2):
        out_ref[:, COLS * h : COLS * (h + 1)] = pltpu.roll(total[:, COLS * h : COLS * (h + 1)], turn, 1)
    for move in moves:
        move.wait_send()


def on_device(left, right, bond_signs, hop):
    wide_size = lax.axis_size("wide")
    narrow_size = lax.axis_size("narrow")
    chips = wide_size // 2
    scale = 1.0 / math.sqrt(ROWS * COLS * wide_size * narrow_size)
    hbm = pl.BlockSpec(memory_space=pl.ANY)
    dma = pltpu.SemaphoreType.DMA
    block = (8, OPS * VECS)
    spread = pl.pallas_call(
        functools.partial(moments_kernel, scale, chips),
        out_shape=jax.ShapeDtypeStruct(block, F32),
        in_specs=[hbm] * 4,
        out_specs=pl.BlockSpec(memory_space=pltpu.VMEM),
        scratch_shapes=[
            pltpu.VMEM((VECS, ROWS, COLS), BF16),
            pltpu.VMEM((VECS, ROWS, COLS), BF16),
            pltpu.VMEM((OPS, 2 * RANGE, ROWS, COLS), jnp.int32),
            pltpu.SMEM((OPS, RANGE), F32),
            pltpu.VMEM((VECS * PITCH, COLS), F32),
            pltpu.VMEM((ROWS + 2 * RANGE, VECS, COLS), F32),
            pltpu.VMEM((ROWS + 2 * RANGE, VECS, COLS), F32),
            pltpu.VMEM((ROWS, VECS, COLS), BF16),
            pltpu.VMEM((ROWS, VECS, COLS), BF16),
            pltpu.VMEM((8 * OPS, ROWS + 16, COLS), F32),
            pltpu.VMEM((16, ROWS, COLS), F32),
            pltpu.VMEM((2 * COLS, 8 * COLS), BF16),
            pltpu.VMEM((RANGE, VECS, COLS), BF16),
            pltpu.VMEM((RANGE, VECS, COLS), BF16),
            pltpu.VMEM((ROWS // 2, OPS * VECS, 2 * COLS), BF16),
            pltpu.VMEM((2, OPS * VECS, COLS), F32),
            pltpu.VMEM((2, 2, RANGE, VECS, COLS), BF16),
            pltpu.VMEM((2, 2, RANGE, VECS, COLS), BF16),
            pltpu.VMEM((2, 2, COLS // 2, 2 * COLS), BF16),
            pltpu.VMEM((2, 2, COLS // 2, 2 * COLS), BF16),
            pltpu.VMEM((2, 8 * RANGE, COLS), F32),
            pltpu.VMEM((2, 8 * RANGE, COLS), BF16),
            pltpu.VMEM((2, 8 * RANGE, COLS), BF16),
            pltpu.VMEM((2, ROWS, COLS), BF16),
            pltpu.VMEM((2, ROWS, COLS), BF16),
            pltpu.VMEM((2, chips) + block, F32),
            pltpu.VMEM((chips,) + block, F32),
            pltpu.VMEM((chips,) + block, F32),
            pltpu.VMEM((chips - 1,) + block, F32),
            pltpu.VMEM(block, F32),
            pltpu.VMEM((narrow_size - 1,) + block, F32),
            dma((4,)),
            dma((3, 4)),
            dma((3, 4)),
            dma((1,)),
            dma((1,)),
            dma((chips - 1,)),
            dma((chips - 1,)),
            dma((narrow_size - 1,)),
            dma((narrow_size - 1,)),
        ],
        compiler_params=pltpu.CompilerParams(
            collective_id=0, has_side_effects=True, vmem_limit_bytes=60 << 20
        ),
        name="moments",
    )(left, right, bond_signs, hop)
    wanted = spread.reshape(2, OPS, OPS, VECS)[..., : VECS // narrow_size]
    return wanted.transpose(1, 2, 0, 3).reshape(OPS * OPS, 2, VECS // narrow_size)


def solution(mesh):
    in_specs = (
        P(None, "wide", "narrow"),
        P(None, "wide", "narrow"),
        P(None, None, "wide", "narrow"),
        P(),
    )
    return jax.shard_map(
        on_device, mesh=mesh, in_specs=in_specs, out_specs=P(None, "wide", "narrow"), check_vma=False
    )
```

```python
import functools
import math

import jax
import jax.numpy as jnp
from jax import lax
from jax.experimental import pallas as pl
from jax.experimental.pallas import tpu as pltpu
from jax.sharding import PartitionSpec as P

OPS = 4
RANGE = 4
VECS = 64
ROWS = 64
COLS = 128
PITCH = 72
BANDS = ROWS // RANGE
STEPS = (1, 2, 3, 4, -1, -2, -3, -4)
MESH = pl.DeviceIdType.MESH
F32 = jnp.float32
BF16 = jnp.bfloat16


def iota(shape, dim):
    return lax.broadcasted_iota(jnp.int32, shape, dim)


def ones_where(condition):
    return jnp.where(condition, 1.0, 0.0).astype(BF16)


def moments_kernel(
    scale, chips, left_hbm, right_hbm, bits_hbm, hop_hbm, out_ref,
    left_ref, right_ref, bits_ref, hop_ref,
    flat, field_r, field_l, plain_r, plain_l, weight, weight_adj, shifter, packed_r, packed_l,
    slid, first, back, product,
    row_send, row_recv, col_send, col_recv, sr_stage, sr_send, sr_recv, sc_send, sc_recv,
    parts, own, arrived_core, arrived_wide, whole, arrived_narrow,
    load_sem, send_sem, recv_sem, core_send, core_recv, wide_send, wide_recv, narrow_send, narrow_recv,
):
    loads = [
        pltpu.make_async_copy(source, target, load_sem.at[i])
        for i, (source, target) in enumerate(
            ((right_hbm, right_ref), (bits_hbm, bits_ref), (hop_hbm, hop_ref), (left_hbm, left_ref))
        )
    ]
    for load in loads:
        load.start()

    wide_size = lax.axis_size("wide")
    narrow_size = lax.axis_size("narrow")
    wide = lax.axis_index("wide")
    narrow = lax.axis_index("narrow")
    w_up, w_down = lax.rem(wide + 1, wide_size), lax.rem(wide + wide_size - 1, wide_size)
    n_up, n_down = lax.rem(narrow + 1, narrow_size), lax.rem(narrow + narrow_size - 1, narrow_size)
    sides = ((w_up, narrow), (w_down, narrow), (wide, n_up), (wide, n_down))
    core, chip = lax.rem(wide, 2), wide // 2
    partner = (wide + 1 - 2 * core, narrow)
    in_wide = [(2 * lax.rem(chip + d, chips) + core, narrow) for d in range(1, chips)]
    in_narrow = [(wide, lax.rem(narrow + d, narrow_size)) for d in range(1, narrow_size)]

    barrier = pltpu.get_barrier_semaphore()
    everyone = [sides[0], sides[1]] + in_wide + in_narrow
    for device in everyone:
        pl.semaphore_signal(barrier, inc=1, device_id=device, device_id_type=MESH)

    def remote(source, target, sent, received, device):
        return pltpu.make_async_remote_copy(
            src_ref=source, dst_ref=target, send_sem=sent, recv_sem=received,
            device_id=device, device_id_type=MESH,
        )

    kappa = iota((2 * COLS, COLS), 0)
    tail = kappa - COLS
    edge = jnp.where(tail < COLS // 2, tail % RANGE - RANGE, tail % RANGE + COLS)
    origin = jnp.where(kappa < COLS, kappa, edge) - iota((2 * COLS, COLS), 1)
    for t, step in enumerate(STEPS):
        shifter[:, COLS * t : COLS * (t + 1)] = ones_where(origin == step)

    spot_row = iota((COLS, 2 * COLS), 0)
    spot_band = spot_row % (COLS // 2) // RANGE
    spot_col = spot_row % RANGE + jnp.where(spot_row < COLS // 2, COLS - RANGE, 0)
    spot_lane = COLS * spot_band + spot_col - iota((COLS, 2 * COLS), 1)

    def transposed(source, field, plain):
        @pl.loop(0, VECS)
        def _(v):
            flat[pl.ds(pl.multiple_of(v * PITCH, 8), ROWS), :] = source[v].astype(F32)

        @pl.loop(0, ROWS)
        def _(row):
            groups = [flat[pl.ds(8 * g * PITCH + row, 8, stride=PITCH), :] for g in range(VECS // 8)]
            whole_row = jnp.concatenate(groups, axis=0)
            field[row + RANGE] = whole_row
            plain[row] = whole_row.astype(BF16)

    def edges(side, plain):
        row_send[side, 0] = plain[ROWS - RANGE : ROWS]
        row_send[side, 1] = plain[0:RANGE]
        picked = jnp.zeros((COLS, 2 * COLS), F32)
        for c in range(BANDS // 2):
            pick = ones_where(spot_lane == 2 * COLS * c)
            bands = [
                plain[RANGE * b : RANGE * (b + 1)].reshape(RANGE * VECS, COLS)
                for b in (2 * c, 2 * c + 1)
            ]
            picked = picked + lax.dot_general(
                pick, jnp.concatenate(bands, axis=1), (((1,), (1,)), ((), ())),
                preferred_element_type=F32,
            )
        col_send[side, 0] = picked[: COLS // 2].astype(BF16)
        col_send[side, 1] = picked[COLS // 2 :].astype(BF16)

    def copies(slot, row_pair, col_pair):
        made = []
        for way in range(4):
            (source, target), part = (row_pair, way) if way < 2 else (col_pair, way - 2)
            made.append(
                remote(
                    source.at[part], target.at[part], send_sem.at[slot, way], recv_sem.at[slot, way],
                    sides[way],
                )
            )
        return made

    def landed(side, field, packed, moves):
        for move in moves:
            move.wait_recv()
        field[0:RANGE] = row_recv[side, 0].astype(F32)
        field[ROWS + RANGE : ROWS + 2 * RANGE] = row_recv[side, 1].astype(F32)
        strips = jnp.concatenate([col_recv[side, way].astype(F32) for way in range(2)], axis=0)
        packed[...] = jnp.transpose(strips).astype(BF16).reshape(RANGE, VECS, COLS)

    loads[0].wait()
    transposed(right_ref, field_r, plain_r)
    edges(0, plain_r)
    pl.semaphore_wait(barrier, len(everyone))
    moves_r = copies(0, (row_send.at[0], row_recv.at[0]), (col_send.at[0], col_recv.at[0]))
    for move in moves_r:
        move.start()

    loads[3].wait()
    transposed(left_ref, field_l, plain_l)
    edges(1, plain_l)
    moves_l = copies(1, (row_send.at[1], row_recv.at[1]), (col_send.at[1], col_recv.at[1]))
    for move in moves_l:
        move.start()

    loads[1].wait()
    loads[2].wait()

    def coefficient(op, tap):
        return hop_ref[op, tap % RANGE] * (1.0 if tap < RANGE else -1.0)

    def sign_of(op, tap):
        return (2 * bits_ref[op, tap] - 1).astype(F32)

    small = iota((ROWS, COLS), 1)
    for half, op in enumerate((0, 2)):
        for tap in range(2 * RANGE):
            sign = sign_of(op, tap)
            weight[8 * op + tap, 8 : 8 + ROWS, :] = coefficient(op, tap) * sign
            way, at = (0, ROWS - RANGE) if tap < RANGE else (1, 0)
            spot = (4 * half + tap % RANGE) * RANGE
            sr_stage[way, spot : spot + RANGE, :] = sign[at : at + RANGE]
    for way in range(2):
        sr_send[way] = sr_stage[way].astype(BF16)
    for way in range(2):
        held = jnp.zeros((ROWS, COLS), F32)
        for half, op in enumerate((1, 3)):
            for k in range(RANGE):
                tap = RANGE * way + k
                sign = sign_of(op, tap)
                weight[8 * op + tap, 8 : 8 + ROWS, :] = coefficient(op, tap) * sign
                at = COLS // 2 * way + RANGE * (4 * half + k)
                moved = pltpu.roll(sign, at + RANGE if way == 0 else at, 1) if at or way == 0 else sign
                held = jnp.where(small // RANGE == at // RANGE, moved, held)
        sc_send[way] = held.astype(BF16)
    moves_s = copies(2, (sr_send, sr_recv), (sc_send, sc_recv))
    for move in moves_s:
        move.start()

    def along_rows(field, row, adjoint):
        sums = [None, None]
        for tap in range(2 * RANGE):
            step = -STEPS[tap] if adjoint else STEPS[tap]
            x = field[RANGE + row + step]
            for half, op in enumerate((0, 2)):
                at = 8 + row + (step if adjoint else 0)
                term = weight[8 * op + tap, pl.ds(at, 1), :] * x
                sums[half] = term if sums[half] is None else sums[half] + term
        return sums

    wide_lane = iota((VECS, COLS), 1) % (COLS // 2) // RANGE

    def shift_cols(plain, packed, band):
        inside = wide_lane == band
        rows = []
        for j in range(RANGE):
            strip = packed[j]
            rows.append(
                jnp.concatenate([plain[RANGE * band + j], jnp.where(inside, strip, jnp.zeros_like(strip))], axis=1)
            )
        lhs = jnp.concatenate(rows, axis=0)
        for t in range(4):
            at = slice(2 * COLS * t, 2 * COLS * (t + 1))
            slid[:, at] = jnp.dot(lhs, shifter[:, at], preferred_element_type=F32)

    def along_cols(j, row, adjoint):
        sums = [None, None]
        for t in range(2 * RANGE):
            tap = (t + RANGE) % (2 * RANGE) if adjoint else t
            x = slid[VECS * j : VECS * (j + 1), COLS * t : COLS * (t + 1)]
            for half, op in enumerate((1, 3)):
                if adjoint:
                    w = weight_adj[8 * half + tap, pl.ds(row, 1), :]
                else:
                    w = weight[8 * op + tap, pl.ds(8 + row, 1), :]
                term = w * x
                sums[half] = term if sums[half] is None else sums[half] + term
        return sums

    def applied(field, band, adjoint, store):
        for j in range(RANGE):
            row = RANGE * band + j
            even = along_rows(field, row, adjoint)
            odd = along_cols(j, row, adjoint)
            for op in range(OPS):
                value = (odd if op % 2 else even)[op // 2]
                store(slice(VECS * op, VECS * (op + 1)), slice(COLS * j, COLS * (j + 1)), value.astype(BF16))

    for move in moves_r:
        move.wait_send()
    landed(0, field_r, packed_r, moves_r)

    shift_cols(plain_r, packed_r, 0)

    @pl.loop(0, BANDS)
    def _(band):
        def store(vecs, cols, value):
            first[band, vecs, cols] = value

        applied(field_r, band, False, store)
        shift_cols(plain_r, packed_r, jnp.minimum(band + 1, BANDS - 1))

    for move in moves_l + moves_s:
        move.wait_send()
    for move in moves_s:
        move.wait_recv()
    landed(1, field_l, packed_l, moves_l)

    for way in range(2):
        sr_stage[way] = sr_recv[way].astype(F32)
    for half, op in enumerate((0, 2)):
        for tap in range(2 * RANGE):
            way, at = (0, 8 - RANGE) if tap < RANGE else (1, 8 + ROWS)
            spot = (4 * half + tap % RANGE) * RANGE
            weight[8 * op + tap, at : at + RANGE, :] = coefficient(op, tap) * sr_stage[way, spot : spot + RANGE, :]
    strips = sc_recv[0].astype(F32) + sc_recv[1].astype(F32)
    for tap in range(2 * RANGE):
        lhs = []
        for half, op in enumerate((1, 3)):
            spot = 4 * half + tap % RANGE
            inside = small % (COLS // 2) // RANGE == spot
            lhs.append(jnp.concatenate([sign_of(op, tap), jnp.where(inside, strips, 0.0)], axis=1))
        t = (tap + RANGE) % (2 * RANGE)
        moved = jnp.dot(
            jnp.concatenate(lhs, axis=0).astype(BF16), shifter[:, COLS * t : COLS * (t + 1)],
            preferred_element_type=F32,
        )
        for half, op in enumerate((1, 3)):
            weight_adj[8 * half + tap] = coefficient(op, tap) * moved[ROWS * half : ROWS * (half + 1)]

    product[...] = jnp.zeros_like(product)
    back[...] = jnp.zeros_like(back)

    def gram(band):
        part = lax.dot_general(back[...], first[band], (((1,), (1,)), ((), ())), preferred_element_type=F32)
        for h in range(2):
            product[h] += part[:, COLS * h : COLS * (h + 1)]

    shift_cols(plain_l, packed_l, 0)

    @pl.loop(0, BANDS)
    def _(band):
        def store(vecs, cols, value):
            back[vecs, cols] = value

        gram(jnp.maximum(band - 1, 0))
        applied(field_l, band, True, store)
        shift_cols(plain_l, packed_l, jnp.minimum(band + 1, BANDS - 1))

    gram(BANDS - 1)

    @pl.loop(0, VECS // 2)
    def _(block):
        for h in range(2):
            for i in range(2):
                parts[block % 2, block // 2, 4 * i : 4 * i + 4, COLS * h : COLS * (h + 1)] = scale * product[
                    h, pl.ds(2 * block + i, 4, stride=VECS), :
                ]

    swap = remote(parts.at[1 - core], arrived_core, core_send.at[0], core_recv.at[0], partner)
    swap.start()
    swap.wait()
    own[...] = parts[core] + arrived_core[...]

    moves = []
    for d, device in enumerate(in_wide):
        target = lax.rem(chip + d + 1, chips)
        moves.append(remote(own.at[target], arrived_wide.at[d], wide_send.at[d], wide_recv.at[d], device))
    for move in moves:
        move.start()
    for move in moves:
        move.wait_recv()
    total = own[chip]
    for d in range(chips - 1):
        total = total + arrived_wide[d]
    whole[...] = total
    for move in moves:
        move.wait_send()

    moves = []
    for d, device in enumerate(in_narrow):
        moves.append(remote(whole, arrived_narrow.at[d], narrow_send.at[d], narrow_recv.at[d], device))
    for move in moves:
        move.start()
    for move in moves:
        move.wait_recv()
    total = whole[...]
    for d in range(narrow_size - 1):
        total = total + arrived_narrow[d]
    turn = lax.rem(COLS - 8 * narrow, COLS)
    for h in range(2):
        out_ref[:, COLS * h : COLS * (h + 1)] = pltpu.roll(total[:, COLS * h : COLS * (h + 1)], turn, 1)
    for move in moves:
        move.wait_send()


def on_device(left, right, bond_signs, hop):
    wide_size = lax.axis_size("wide")
    narrow_size = lax.axis_size("narrow")
    chips = wide_size // 2
    scale = 1.0 / math.sqrt(ROWS * COLS * wide_size * narrow_size)
    hbm = pl.BlockSpec(memory_space=pl.ANY)
    dma = pltpu.SemaphoreType.DMA
    block = (8, OPS * VECS)
    spread = pl.pallas_call(
        functools.partial(moments_kernel, scale, chips),
        out_shape=jax.ShapeDtypeStruct(block, F32),
        in_specs=[hbm] * 4,
        out_specs=pl.BlockSpec(memory_space=pltpu.VMEM),
        scratch_shapes=[
            pltpu.VMEM((VECS, ROWS, COLS), BF16),
            pltpu.VMEM((VECS, ROWS, COLS), BF16),
            pltpu.VMEM((OPS, 2 * RANGE, ROWS, COLS), jnp.int32),
            pltpu.SMEM((OPS, RANGE), F32),
            pltpu.VMEM((VECS * PITCH, COLS), F32),
            pltpu.VMEM((ROWS + 2 * RANGE, VECS, COLS), F32),
            pltpu.VMEM((ROWS + 2 * RANGE, VECS, COLS), F32),
            pltpu.VMEM((ROWS, VECS, COLS), BF16),
            pltpu.VMEM((ROWS, VECS, COLS), BF16),
            pltpu.VMEM((8 * OPS, ROWS + 16, COLS), F32),
            pltpu.VMEM((16, ROWS, COLS), F32),
            pltpu.VMEM((2 * COLS, 8 * COLS), BF16),
            pltpu.VMEM((RANGE, VECS, COLS), BF16),
            pltpu.VMEM((RANGE, VECS, COLS), BF16),
            pltpu.VMEM((RANGE * VECS, 8 * COLS), F32),
            pltpu.VMEM((BANDS, OPS * VECS, RANGE * COLS), BF16),
            pltpu.VMEM((OPS * VECS, RANGE * COLS), BF16),
            pltpu.VMEM((2, OPS * VECS, COLS), F32),
            pltpu.VMEM((2, 2, RANGE, VECS, COLS), BF16),
            pltpu.VMEM((2, 2, RANGE, VECS, COLS), BF16),
            pltpu.VMEM((2, 2, COLS // 2, 2 * COLS), BF16),
            pltpu.VMEM((2, 2, COLS // 2, 2 * COLS), BF16),
            pltpu.VMEM((2, 8 * RANGE, COLS), F32),
            pltpu.VMEM((2, 8 * RANGE, COLS), BF16),
            pltpu.VMEM((2, 8 * RANGE, COLS), BF16),
            pltpu.VMEM((2, ROWS, COLS), BF16),
            pltpu.VMEM((2, ROWS, COLS), BF16),
            pltpu.VMEM((2, chips) + block, F32),
            pltpu.VMEM((chips,) + block, F32),
            pltpu.VMEM((chips,) + block, F32),
            pltpu.VMEM((chips - 1,) + block, F32),
            pltpu.VMEM(block, F32),
            pltpu.VMEM((narrow_size - 1,) + block, F32),
            dma((4,)),
            dma((3, 4)),
            dma((3, 4)),
            dma((1,)),
            dma((1,)),
            dma((chips - 1,)),
            dma((chips - 1,)),
            dma((narrow_size - 1,)),
            dma((narrow_size - 1,)),
        ],
        compiler_params=pltpu.CompilerParams(
            collective_id=0, has_side_effects=True, vmem_limit_bytes=60 << 20
        ),
        name="moments",
    )(left, right, bond_signs, hop)
    wanted = spread.reshape(2, OPS, OPS, VECS)[..., : VECS // narrow_size]
    return wanted.transpose(1, 2, 0, 3).reshape(OPS * OPS, 2, VECS // narrow_size)


def solution(mesh):
    in_specs = (
        P(None, "wide", "narrow"),
        P(None, "wide", "narrow"),
        P(None, None, "wide", "narrow"),
        P(),
    )
    return jax.shard_map(
        on_device, mesh=mesh, in_specs=in_specs, out_specs=P(None, "wide", "narrow"), check_vma=False
    )
```

```python
import functools
import math

import jax
import jax.numpy as jnp
from jax import lax
from jax.experimental import pallas as pl
from jax.experimental.pallas import tpu as pltpu
from jax.sharding import PartitionSpec as P

OPS = 4
RANGE = 4
VECS = 64
ROWS = 64
COLS = 128
PITCH = 72
BANDS = ROWS // RANGE
STEPS = (1, 2, 3, 4, -1, -2, -3, -4)
MESH = pl.DeviceIdType.MESH
F32 = jnp.float32
BF16 = jnp.bfloat16


def iota(shape, dim):
    return lax.broadcasted_iota(jnp.int32, shape, dim)


def ones_where(condition):
    return jnp.where(condition, 1.0, 0.0).astype(BF16)


def moments_kernel(
    scale, chips, left_hbm, right_hbm, bits_hbm, hop_hbm, out_ref,
    left_ref, right_ref, bits_ref, hop_ref,
    flat, field_r, field_l, plain_r, plain_l, weight, weight_adj, shifter, packed_r, packed_l,
    slid, first, back, product,
    row_send, row_recv, col_send, col_recv, sr_stage, sr_send, sr_recv, sc_send, sc_recv,
    parts, own, arrived_core, arrived_wide, whole, arrived_narrow,
    load_sem, send_sem, recv_sem, core_send, core_recv, wide_send, wide_recv, narrow_send, narrow_recv,
):
    loads = [
        pltpu.make_async_copy(source, target, load_sem.at[i])
        for i, (source, target) in enumerate(
            ((right_hbm, right_ref), (bits_hbm, bits_ref), (hop_hbm, hop_ref), (left_hbm, left_ref))
        )
    ]
    for load in loads:
        load.start()

    wide_size = lax.axis_size("wide")
    narrow_size = lax.axis_size("narrow")
    wide = lax.axis_index("wide")
    narrow = lax.axis_index("narrow")
    w_up, w_down = lax.rem(wide + 1, wide_size), lax.rem(wide + wide_size - 1, wide_size)
    n_up, n_down = lax.rem(narrow + 1, narrow_size), lax.rem(narrow + narrow_size - 1, narrow_size)
    sides = ((w_up, narrow), (w_down, narrow), (wide, n_up), (wide, n_down))
    core, chip = lax.rem(wide, 2), wide // 2
    partner = (wide + 1 - 2 * core, narrow)
    wide_steps = sorted(range(1, chips), key=lambda d: -min(d, chips - d))
    narrow_steps = sorted(range(1, narrow_size), key=lambda d: -min(d, narrow_size - d))
    in_wide = [(2 * lax.rem(chip + d, chips) + core, narrow) for d in wide_steps]
    in_narrow = [(wide, lax.rem(narrow + d, narrow_size)) for d in narrow_steps]

    barrier = pltpu.get_barrier_semaphore()
    everyone = [sides[0], sides[1]] + in_wide + in_narrow
    for device in everyone:
        pl.semaphore_signal(barrier, inc=1, device_id=device, device_id_type=MESH)

    def remote(source, target, sent, received, device):
        return pltpu.make_async_remote_copy(
            src_ref=source, dst_ref=target, send_sem=sent, recv_sem=received,
            device_id=device, device_id_type=MESH,
        )

    kappa = iota((2 * COLS, COLS), 0)
    tail = kappa - COLS
    edge = jnp.where(tail < COLS // 2, tail % RANGE - RANGE, tail % RANGE + COLS)
    origin = jnp.where(kappa < COLS, kappa, edge) - iota((2 * COLS, COLS), 1)
    for t, step in enumerate(STEPS):
        shifter[:, COLS * t : COLS * (t + 1)] = ones_where(origin == step)

    spot_row = iota((COLS, 2 * COLS), 0)
    spot_band = spot_row % (COLS // 2) // RANGE
    spot_col = spot_row % RANGE + jnp.where(spot_row < COLS // 2, COLS - RANGE, 0)
    spot_lane = COLS * spot_band + spot_col - iota((COLS, 2 * COLS), 1)

    def transposed(source, field, plain):
        @pl.loop(0, VECS, unroll=4)
        def _(v):
            flat[pl.ds(pl.multiple_of(v * PITCH, 8), ROWS), :] = source[v].astype(F32)

        @pl.loop(0, ROWS, unroll=4)
        def _(row):
            groups = [flat[pl.ds(8 * g * PITCH + row, 8, stride=PITCH), :] for g in range(VECS // 8)]
            whole_row = jnp.concatenate(groups, axis=0)
            field[row + RANGE] = whole_row
            plain[row] = whole_row.astype(BF16)

    def edges(side, plain):
        row_send[side, 0] = plain[ROWS - RANGE : ROWS]
        row_send[side, 1] = plain[0:RANGE]
        sums = [jnp.zeros((COLS, 2 * COLS), F32) for _ in range(2)]
        for c in range(BANDS // 2):
            pick = ones_where(spot_lane == 2 * COLS * c)
            bands = [
                plain[RANGE * b : RANGE * (b + 1)].reshape(RANGE * VECS, COLS)
                for b in (2 * c, 2 * c + 1)
            ]
            sums[c % 2] = sums[c % 2] + lax.dot_general(
                pick, jnp.concatenate(bands, axis=1), (((1,), (1,)), ((), ())),
                preferred_element_type=F32,
            )
        picked = sums[0] + sums[1]
        col_send[side, 0] = picked[: COLS // 2].astype(BF16)
        col_send[side, 1] = picked[COLS // 2 :].astype(BF16)

    def copies(slot, row_pair, col_pair):
        made = []
        for way in range(4):
            (source, target), part = (row_pair, way) if way < 2 else (col_pair, way - 2)
            made.append(
                remote(
                    source.at[part], target.at[part], send_sem.at[slot, way], recv_sem.at[slot, way],
                    sides[way],
                )
            )
        return made

    def landed(side, field, packed, moves):
        for move in moves:
            move.wait_recv()
        field[0:RANGE] = row_recv[side, 0].astype(F32)
        field[ROWS + RANGE : ROWS + 2 * RANGE] = row_recv[side, 1].astype(F32)
        strips = jnp.concatenate([col_recv[side, way].astype(F32) for way in range(2)], axis=0)
        packed[...] = jnp.transpose(strips).astype(BF16).reshape(RANGE, VECS, COLS)

    loads[0].wait()
    transposed(right_ref, field_r, plain_r)
    edges(0, plain_r)
    pl.semaphore_wait(barrier, len(everyone))
    moves_r = copies(0, (row_send.at[0], row_recv.at[0]), (col_send.at[0], col_recv.at[0]))
    for move in moves_r:
        move.start()

    loads[3].wait()
    transposed(left_ref, field_l, plain_l)
    edges(1, plain_l)
    moves_l = copies(1, (row_send.at[1], row_recv.at[1]), (col_send.at[1], col_recv.at[1]))
    for move in moves_l:
        move.start()

    loads[1].wait()
    loads[2].wait()

    def coefficient(op, tap):
        return hop_ref[op, tap % RANGE] * (1.0 if tap < RANGE else -1.0)

    def sign_of(op, tap):
        return (2 * bits_ref[op, tap] - 1).astype(F32)

    small = iota((ROWS, COLS), 1)
    for half, op in enumerate((0, 2)):
        for tap in range(2 * RANGE):
            sign = sign_of(op, tap)
            weight[8 * op + tap, 8 : 8 + ROWS, :] = coefficient(op, tap) * sign
            way, at = (0, ROWS - RANGE) if tap < RANGE else (1, 0)
            spot = (4 * half + tap % RANGE) * RANGE
            sr_stage[way, spot : spot + RANGE, :] = sign[at : at + RANGE]
    for way in range(2):
        sr_send[way] = sr_stage[way].astype(BF16)
    for way in range(2):
        held = jnp.zeros((ROWS, COLS), F32)
        for half, op in enumerate((1, 3)):
            for k in range(RANGE):
                tap = RANGE * way + k
                sign = sign_of(op, tap)
                weight[8 * op + tap, 8 : 8 + ROWS, :] = coefficient(op, tap) * sign
                at = COLS // 2 * way + RANGE * (4 * half + k)
                moved = pltpu.roll(sign, at + RANGE if way == 0 else at, 1) if at or way == 0 else sign
                held = jnp.where(small // RANGE == at // RANGE, moved, held)
        sc_send[way] = held.astype(BF16)
    moves_s = copies(2, (sr_send, sr_recv), (sc_send, sc_recv))
    for move in moves_s:
        move.start()

    def along_rows(field, row, adjoint):
        sums = [None, None]
        for tap in range(2 * RANGE):
            step = -STEPS[tap] if adjoint else STEPS[tap]
            x = field[RANGE + row + step]
            for half, op in enumerate((0, 2)):
                at = 8 + row + (step if adjoint else 0)
                term = weight[8 * op + tap, pl.ds(at, 1), :] * x
                sums[half] = term if sums[half] is None else sums[half] + term
        return sums

    wide_lane = iota((VECS, COLS), 1) % (COLS // 2) // RANGE

    def shift_cols(plain, packed, band, slot):
        inside = wide_lane == band
        rows = []
        for j in range(RANGE):
            strip = packed[j]
            rows.append(
                jnp.concatenate([plain[RANGE * band + j], jnp.where(inside, strip, jnp.zeros_like(strip))], axis=1)
            )
        lhs = jnp.concatenate(rows, axis=0)
        for t in range(4):
            at = slice(2 * COLS * t, 2 * COLS * (t + 1))
            slid[slot, :, at] = jnp.dot(lhs, shifter[:, at], preferred_element_type=F32)

    def along_cols(slot, j, row, adjoint):
        sums = [None, None]
        for t in range(2 * RANGE):
            tap = (t + RANGE) % (2 * RANGE) if adjoint else t
            x = slid[slot, VECS * j : VECS * (j + 1), COLS * t : COLS * (t + 1)]
            for half, op in enumerate((1, 3)):
                if adjoint:
                    w = weight_adj[8 * half + tap, pl.ds(row, 1), :]
                else:
                    w = weight[8 * op + tap, pl.ds(8 + row, 1), :]
                term = w * x
                sums[half] = term if sums[half] is None else sums[half] + term
        return sums

    def applied(field, band, slot, adjoint, store):
        for j in range(RANGE):
            row = RANGE * band + j
            even = along_rows(field, row, adjoint)
            odd = along_cols(slot, j, row, adjoint)
            for op in range(OPS):
                value = (odd if op % 2 else even)[op // 2]
                store(slice(VECS * op, VECS * (op + 1)), slice(COLS * j, COLS * (j + 1)), value.astype(BF16))

    landed(0, field_r, packed_r, moves_r)

    shift_cols(plain_r, packed_r, 0, 0)

    @pl.loop(0, BANDS // 2)
    def _(couple):
        for slot in range(2):
            band = 2 * couple + slot

            def store(vecs, cols, value):
                first[band, vecs, cols] = value

            shift_cols(plain_r, packed_r, jnp.minimum(band + 1, BANDS - 1), 1 - slot)
            applied(field_r, band, slot, False, store)

    for move in moves_s:
        move.wait_recv()
    landed(1, field_l, packed_l, moves_l)

    for way in range(2):
        sr_stage[way] = sr_recv[way].astype(F32)
    for half, op in enumerate((0, 2)):
        for tap in range(2 * RANGE):
            way, at = (0, 8 - RANGE) if tap < RANGE else (1, 8 + ROWS)
            spot = (4 * half + tap % RANGE) * RANGE
            weight[8 * op + tap, at : at + RANGE, :] = coefficient(op, tap) * sr_stage[way, spot : spot + RANGE, :]
    strips = sc_recv[0].astype(F32) + sc_recv[1].astype(F32)
    for tap in range(2 * RANGE):
        lhs = []
        for half, op in enumerate((1, 3)):
            spot = 4 * half + tap % RANGE
            inside = small % (COLS // 2) // RANGE == spot
            lhs.append(jnp.concatenate([sign_of(op, tap), jnp.where(inside, strips, 0.0)], axis=1))
        t = (tap + RANGE) % (2 * RANGE)
        moved = jnp.dot(
            jnp.concatenate(lhs, axis=0).astype(BF16), shifter[:, COLS * t : COLS * (t + 1)],
            preferred_element_type=F32,
        )
        for half, op in enumerate((1, 3)):
            weight_adj[8 * half + tap] = coefficient(op, tap) * moved[ROWS * half : ROWS * (half + 1)]

    product[...] = jnp.zeros_like(product)
    back[...] = jnp.zeros_like(back)

    def gram(band, slot):
        part = lax.dot_general(back[slot], first[band], (((1,), (1,)), ((), ())), preferred_element_type=F32)
        for h in range(2):
            product[h] += part[:, COLS * h : COLS * (h + 1)]

    shift_cols(plain_l, packed_l, 0, 0)

    @pl.loop(0, BANDS // 2)
    def _(couple):
        for slot in range(2):
            band = 2 * couple + slot

            def store(vecs, cols, value):
                back[slot, vecs, cols] = value

            applied(field_l, band, slot, True, store)
            shift_cols(plain_l, packed_l, jnp.minimum(band + 1, BANDS - 1), 1 - slot)
            gram(jnp.maximum(band - 1, 0), 1 - slot)

    gram(BANDS - 1, 1)

    @pl.loop(0, VECS // 2)
    def _(block):
        for h in range(2):
            for i in range(2):
                parts[block % 2, block // 2, 4 * i : 4 * i + 4, COLS * h : COLS * (h + 1)] = scale * product[
                    h, pl.ds(2 * block + i, 4, stride=VECS), :
                ]

    swap = remote(parts.at[1 - core], arrived_core, core_send.at[0], core_recv.at[0], partner)
    swap.start()
    swap.wait()
    own[...] = parts[core] + arrived_core[...]

    moves = []
    for d, device in enumerate(in_wide):
        target = lax.rem(chip + wide_steps[d], chips)
        moves.append(remote(own.at[target], arrived_wide.at[d], wide_send.at[d], wide_recv.at[d], device))
    for move in moves:
        move.start()
    for move in moves:
        move.wait_recv()
    total = own[chip]
    for d in range(chips - 1):
        total = total + arrived_wide[d]
    whole[...] = total
    for move in moves:
        move.wait_send()

    moves = []
    for d, device in enumerate(in_narrow):
        moves.append(remote(whole, arrived_narrow.at[d], narrow_send.at[d], narrow_recv.at[d], device))
    for move in moves:
        move.start()
    for move in moves:
        move.wait_recv()
    total = whole[...]
    for d in range(narrow_size - 1):
        total = total + arrived_narrow[d]
    for b in range(OPS):
        turn = lax.rem(2 * COLS - VECS * (b % 2) - 8 * narrow, COLS)
        mine = pltpu.roll(total[:, COLS * (b // 2) : COLS * (b // 2 + 1)], turn, 1)
        for i in range(2):
            out_ref[i, pl.ds(b, OPS, stride=OPS), :] = mine[OPS * i : OPS * (i + 1)]
    for move in moves + moves_r + moves_l + moves_s:
        move.wait_send()


def on_device(left, right, bond_signs, hop):
    wide_size = lax.axis_size("wide")
    narrow_size = lax.axis_size("narrow")
    chips = wide_size // 2
    scale = 1.0 / math.sqrt(ROWS * COLS * wide_size * narrow_size)
    hbm = pl.BlockSpec(memory_space=pl.ANY)
    dma = pltpu.SemaphoreType.DMA
    block = (8, OPS * VECS)
    spread = pl.pallas_call(
        functools.partial(moments_kernel, scale, chips),
        out_shape=jax.ShapeDtypeStruct((2, OPS * OPS, COLS), F32),
        in_specs=[hbm] * 4,
        out_specs=pl.BlockSpec(memory_space=pltpu.VMEM),
        scratch_shapes=[
            pltpu.VMEM((VECS, ROWS, COLS), BF16),
            pltpu.VMEM((VECS, ROWS, COLS), BF16),
            pltpu.VMEM((OPS, 2 * RANGE, ROWS, COLS), jnp.int32),
            pltpu.SMEM((OPS, RANGE), F32),
            pltpu.VMEM((VECS * PITCH, COLS), F32),
            pltpu.VMEM((ROWS + 2 * RANGE, VECS, COLS), F32),
            pltpu.VMEM((ROWS + 2 * RANGE, VECS, COLS), F32),
            pltpu.VMEM((ROWS, VECS, COLS), BF16),
            pltpu.VMEM((ROWS, VECS, COLS), BF16),
            pltpu.VMEM((8 * OPS, ROWS + 16, COLS), F32),
            pltpu.VMEM((16, ROWS, COLS), F32),
            pltpu.VMEM((2 * COLS, 8 * COLS), BF16),
            pltpu.VMEM((RANGE, VECS, COLS), BF16),
            pltpu.VMEM((RANGE, VECS, COLS), BF16),
            pltpu.VMEM((2, RANGE * VECS, 8 * COLS), F32),
            pltpu.VMEM((BANDS, OPS * VECS, RANGE * COLS), BF16),
            pltpu.VMEM((2, OPS * VECS, RANGE * COLS), BF16),
            pltpu.VMEM((2, OPS * VECS, COLS), F32),
            pltpu.VMEM((2, 2, RANGE, VECS, COLS), BF16),
            pltpu.VMEM((2, 2, RANGE, VECS, COLS), BF16),
            pltpu.VMEM((2, 2, COLS // 2, 2 * COLS), BF16),
            pltpu.VMEM((2, 2, COLS // 2, 2 * COLS), BF16),
            pltpu.VMEM((2, 8 * RANGE, COLS), F32),
            pltpu.VMEM((2, 8 * RANGE, COLS), BF16),
            pltpu.VMEM((2, 8 * RANGE, COLS), BF16),
            pltpu.VMEM((2, ROWS, COLS), BF16),
            pltpu.VMEM((2, ROWS, COLS), BF16),
            pltpu.VMEM((2, chips) + block, F32),
            pltpu.VMEM((chips,) + block, F32),
            pltpu.VMEM((chips,) + block, F32),
            pltpu.VMEM((chips - 1,) + block, F32),
            pltpu.VMEM(block, F32),
            pltpu.VMEM((narrow_size - 1,) + block, F32),
            dma((4,)),
            dma((3, 4)),
            dma((3, 4)),
            dma((1,)),
            dma((1,)),
            dma((chips - 1,)),
            dma((chips - 1,)),
            dma((narrow_size - 1,)),
            dma((narrow_size - 1,)),
        ],
        compiler_params=pltpu.CompilerParams(
            collective_id=0, has_side_effects=True, vmem_limit_bytes=60 << 20
        ),
        name="moments",
    )(left, right, bond_signs, hop)
    return spread[:, :, : VECS // narrow_size].transpose(1, 0, 2)


def solution(mesh):
    in_specs = (
        P(None, "wide", "narrow"),
        P(None, "wide", "narrow"),
        P(None, None, "wide", "narrow"),
        P(),
    )
    return jax.shard_map(
        on_device, mesh=mesh, in_specs=in_specs, out_specs=P(None, "wide", "narrow"), check_vma=False
    )
```

```python
import functools
import math

import jax
import jax.numpy as jnp
from jax import lax
from jax.experimental import pallas as pl
from jax.experimental.pallas import tpu as pltpu
from jax.sharding import PartitionSpec as P

OPS = 4
RANGE = 4
VECS = 64
ROWS = 64
COLS = 128
PITCH = 72
BANDS = ROWS // RANGE
STEPS = (1, 2, 3, 4, -1, -2, -3, -4)
MESH = pl.DeviceIdType.MESH
F32 = jnp.float32
BF16 = jnp.bfloat16


def iota(shape, dim):
    return lax.broadcasted_iota(jnp.int32, shape, dim)


def ones_where(condition):
    return jnp.where(condition, 1.0, 0.0).astype(BF16)


def moments_kernel(
    scale, chips, left_hbm, right_hbm, bits_hbm, hop_hbm, out_ref,
    left_ref, right_ref, bits_ref, hop_ref,
    flat, field_r, field_l, plain_r, plain_l, weight, weight_adj, shifter, packed_r, packed_l,
    slid, first, back, product,
    row_send, row_recv, col_send, col_recv, sr_stage, sr_send, sr_recv, sc_send, sc_recv,
    parts, own, arrived_core, arrived_wide, whole, arrived_narrow,
    staged, load_sem, send_sem, recv_sem, core_send, core_recv, wide_send, wide_recv, narrow_send, narrow_recv,
):
    loads = [
        pltpu.make_async_copy(source, target, load_sem.at[i])
        for i, (source, target) in enumerate(
            ((right_hbm, right_ref), (bits_hbm, bits_ref), (hop_hbm, hop_ref), (left_hbm, left_ref))
        )
    ]
    for load in loads:
        load.start()

    wide_size = lax.axis_size("wide")
    narrow_size = lax.axis_size("narrow")
    wide = lax.axis_index("wide")
    narrow = lax.axis_index("narrow")
    w_up, w_down = lax.rem(wide + 1, wide_size), lax.rem(wide + wide_size - 1, wide_size)
    n_up, n_down = lax.rem(narrow + 1, narrow_size), lax.rem(narrow + narrow_size - 1, narrow_size)
    sides = ((w_up, narrow), (w_down, narrow), (wide, n_up), (wide, n_down))
    core, chip = lax.rem(wide, 2), wide // 2
    partner = (wide + 1 - 2 * core, narrow)
    wide_steps = sorted(range(1, chips), key=lambda d: -min(d, chips - d))
    narrow_steps = sorted(range(1, narrow_size), key=lambda d: -min(d, narrow_size - d))
    in_wide = [(2 * lax.rem(chip + d, chips) + core, narrow) for d in wide_steps]
    in_narrow = [(wide, lax.rem(narrow + d, narrow_size)) for d in narrow_steps]

    barrier = pltpu.get_barrier_semaphore()
    everyone = [sides[0], sides[1]] + in_narrow[::-1] + in_wide[::-1]
    for device in everyone:
        pl.semaphore_signal(barrier, inc=1, device_id=device, device_id_type=MESH)

    def remote(source, target, sent, received, device):
        return pltpu.make_async_remote_copy(
            src_ref=source, dst_ref=target, send_sem=sent, recv_sem=received,
            device_id=device, device_id_type=MESH,
        )

    kappa = iota((2 * COLS, COLS), 0)
    tail = kappa - COLS
    edge = jnp.where(tail < COLS // 2, tail % RANGE - RANGE, tail % RANGE + COLS)
    origin = jnp.where(kappa < COLS, kappa, edge) - iota((2 * COLS, COLS), 1)
    for t, step in enumerate(STEPS):
        shifter[:, COLS * t : COLS * (t + 1)] = ones_where(origin == step)

    spot_row = iota((COLS, 2 * COLS), 0)
    spot_band = spot_row % (COLS // 2) // RANGE
    spot_col = spot_row % RANGE + jnp.where(spot_row < COLS // 2, COLS - RANGE, 0)
    spot_lane = COLS * spot_band + spot_col - iota((COLS, 2 * COLS), 1)

    def transposed(source, field, plain):
        @pl.loop(0, VECS, unroll=4)
        def _(v):
            flat[pl.ds(pl.multiple_of(v * PITCH, 8), ROWS), :] = source[v].astype(F32)

        @pl.loop(0, ROWS, unroll=4)
        def _(row):
            groups = [flat[pl.ds(8 * g * PITCH + row, 8, stride=PITCH), :] for g in range(VECS // 8)]
            whole_row = jnp.concatenate(groups, axis=0)
            field[row + RANGE] = whole_row
            plain[row] = whole_row.astype(BF16)

    def edges(side, plain):
        row_send[side, 0] = plain[ROWS - RANGE : ROWS]
        row_send[side, 1] = plain[0:RANGE]
        sums = [jnp.zeros((COLS, 2 * COLS), F32) for _ in range(2)]
        for c in range(BANDS // 2):
            pick = ones_where(spot_lane == 2 * COLS * c)
            bands = [
                plain[RANGE * b : RANGE * (b + 1)].reshape(RANGE * VECS, COLS)
                for b in (2 * c, 2 * c + 1)
            ]
            sums[c % 2] = sums[c % 2] + lax.dot_general(
                pick, jnp.concatenate(bands, axis=1), (((1,), (1,)), ((), ())),
                preferred_element_type=F32,
            )
        picked = sums[0] + sums[1]
        col_send[side, 0] = picked[: COLS // 2].astype(BF16)
        col_send[side, 1] = picked[COLS // 2 :].astype(BF16)

    def copies(slot, row_pair, col_pair):
        made = []
        for way in range(4):
            (source, target), part = (row_pair, way) if way < 2 else (col_pair, way - 2)
            made.append(
                remote(
                    source.at[part], target.at[part], send_sem.at[slot, way], recv_sem.at[slot, way],
                    sides[way],
                )
            )
        return made

    def landed(side, field, packed, moves):
        for move in moves:
            move.wait_recv()
        field[0:RANGE] = row_recv[side, 0].astype(F32)
        field[ROWS + RANGE : ROWS + 2 * RANGE] = row_recv[side, 1].astype(F32)
        strips = jnp.concatenate([col_recv[side, way].astype(F32) for way in range(2)], axis=0)
        packed[...] = jnp.transpose(strips).astype(BF16).reshape(RANGE, VECS, COLS)

    loads[0].wait()
    transposed(right_ref, field_r, plain_r)
    edges(0, plain_r)
    pl.semaphore_wait(barrier, len(everyone))
    moves_r = copies(0, (row_send.at[0], row_recv.at[0]), (col_send.at[0], col_recv.at[0]))
    for move in moves_r:
        move.start()

    loads[3].wait()
    transposed(left_ref, field_l, plain_l)
    edges(1, plain_l)
    moves_l = copies(1, (row_send.at[1], row_recv.at[1]), (col_send.at[1], col_recv.at[1]))
    for move in moves_l:
        move.start()

    loads[1].wait()
    loads[2].wait()

    def coefficient(op, tap):
        return hop_ref[op, tap % RANGE] * (1.0 if tap < RANGE else -1.0)

    def sign_of(op, tap):
        return (2 * bits_ref[op, tap] - 1).astype(F32)

    small = iota((ROWS, COLS), 1)
    for half, op in enumerate((0, 2)):
        for tap in range(2 * RANGE):
            sign = sign_of(op, tap)
            weight[8 * op + tap, 8 : 8 + ROWS, :] = coefficient(op, tap) * sign
            way, at = (0, ROWS - RANGE) if tap < RANGE else (1, 0)
            spot = (4 * half + tap % RANGE) * RANGE
            sr_stage[way, spot : spot + RANGE, :] = sign[at : at + RANGE]
    for way in range(2):
        sr_send[way] = sr_stage[way].astype(BF16)
    for way in range(2):
        held = jnp.zeros((ROWS, COLS), F32)
        for half, op in enumerate((1, 3)):
            for k in range(RANGE):
                tap = RANGE * way + k
                sign = sign_of(op, tap)
                weight[8 * op + tap, 8 : 8 + ROWS, :] = coefficient(op, tap) * sign
                at = COLS // 2 * way + RANGE * (4 * half + k)
                moved = pltpu.roll(sign, at + RANGE if way == 0 else at, 1) if at or way == 0 else sign
                held = jnp.where(small // RANGE == at // RANGE, moved, held)
        sc_send[way] = held.astype(BF16)
    moves_s = copies(2, (sr_send, sr_recv), (sc_send, sc_recv))
    for move in moves_s:
        move.start()

    def along_rows(field, row, adjoint):
        sums = [None, None]
        for tap in range(2 * RANGE):
            step = -STEPS[tap] if adjoint else STEPS[tap]
            x = field[RANGE + row + step]
            for half, op in enumerate((0, 2)):
                at = 8 + row + (step if adjoint else 0)
                term = weight[8 * op + tap, pl.ds(at, 1), :] * x
                sums[half] = term if sums[half] is None else sums[half] + term
        return sums

    wide_lane = iota((VECS, COLS), 1) % (COLS // 2) // RANGE

    def shift_cols(plain, packed, band, slot):
        inside = wide_lane == band
        rows = []
        for j in range(RANGE):
            strip = packed[j]
            rows.append(
                jnp.concatenate([plain[RANGE * band + j], jnp.where(inside, strip, jnp.zeros_like(strip))], axis=1)
            )
        lhs = jnp.concatenate(rows, axis=0)
        for t in range(4):
            at = slice(2 * COLS * t, 2 * COLS * (t + 1))
            slid[slot, :, at] = jnp.dot(lhs, shifter[:, at], preferred_element_type=F32)

    def along_cols(slot, j, row, adjoint):
        sums = [None, None]
        for t in range(2 * RANGE):
            tap = (t + RANGE) % (2 * RANGE) if adjoint else t
            x = slid[slot, VECS * j : VECS * (j + 1), COLS * t : COLS * (t + 1)]
            for half, op in enumerate((1, 3)):
                if adjoint:
                    w = weight_adj[8 * half + tap, pl.ds(row, 1), :]
                else:
                    w = weight[8 * op + tap, pl.ds(8 + row, 1), :]
                term = w * x
                sums[half] = term if sums[half] is None else sums[half] + term
        return sums

    def applied(field, band, slot, adjoint, store):
        for j in range(RANGE):
            row = RANGE * band + j
            even = along_rows(field, row, adjoint)
            odd = along_cols(slot, j, row, adjoint)
            for op in range(OPS):
                value = (odd if op % 2 else even)[op // 2]
                store(slice(VECS * op, VECS * (op + 1)), slice(COLS * j, COLS * (j + 1)), value.astype(BF16))

    def row_ops(band):
        for j in range(RANGE):
            sums = along_rows(field_r, RANGE * band + j, False)
            for half, op in enumerate((0, 2)):
                first[band, VECS * op : VECS * (op + 1), COLS * j : COLS * (j + 1)] = sums[half].astype(BF16)

    def col_ops(band, slot):
        for j in range(RANGE):
            sums = along_cols(slot, j, RANGE * band + j, False)
            for half, op in enumerate((1, 3)):
                first[band, VECS * op : VECS * (op + 1), COLS * j : COLS * (j + 1)] = sums[half].astype(BF16)

    @pl.loop(1, BANDS - 1)
    def _(band):
        row_ops(band)

    landed(0, field_r, packed_r, moves_r)
    shift_cols(plain_r, packed_r, 0, 0)
    for band in (0, BANDS - 1):
        row_ops(band)

    @pl.loop(0, BANDS // 2)
    def _(couple):
        for slot in range(2):
            band = 2 * couple + slot
            col_ops(band, slot)
            shift_cols(plain_r, packed_r, jnp.minimum(band + 1, BANDS - 1), 1 - slot)

    for move in moves_s:
        move.wait_recv()
    landed(1, field_l, packed_l, moves_l)

    for way in range(2):
        sr_stage[way] = sr_recv[way].astype(F32)
    for half, op in enumerate((0, 2)):
        for tap in range(2 * RANGE):
            way, at = (0, 8 - RANGE) if tap < RANGE else (1, 8 + ROWS)
            spot = (4 * half + tap % RANGE) * RANGE
            weight[8 * op + tap, at : at + RANGE, :] = coefficient(op, tap) * sr_stage[way, spot : spot + RANGE, :]
    strips = sc_recv[0].astype(F32) + sc_recv[1].astype(F32)
    for tap in range(2 * RANGE):
        lhs = []
        for half, op in enumerate((1, 3)):
            spot = 4 * half + tap % RANGE
            inside = small % (COLS // 2) // RANGE == spot
            lhs.append(jnp.concatenate([sign_of(op, tap), jnp.where(inside, strips, 0.0)], axis=1))
        t = (tap + RANGE) % (2 * RANGE)
        moved = jnp.dot(
            jnp.concatenate(lhs, axis=0).astype(BF16), shifter[:, COLS * t : COLS * (t + 1)],
            preferred_element_type=F32,
        )
        for half, op in enumerate((1, 3)):
            weight_adj[8 * half + tap] = coefficient(op, tap) * moved[ROWS * half : ROWS * (half + 1)]

    product[...] = jnp.zeros_like(product)
    back[...] = jnp.zeros_like(back)

    def gram(band, slot):
        part = lax.dot_general(back[slot], first[band], (((1,), (1,)), ((), ())), preferred_element_type=F32)
        for h in range(2):
            product[h] += part[:, COLS * h : COLS * (h + 1)]

    shift_cols(plain_l, packed_l, 0, 0)

    @pl.loop(0, BANDS // 2)
    def _(couple):
        for slot in range(2):
            band = 2 * couple + slot

            def store(vecs, cols, value):
                back[slot, vecs, cols] = value

            applied(field_l, band, slot, True, store)
            shift_cols(plain_l, packed_l, jnp.minimum(band + 1, BANDS - 1), 1 - slot)
            gram(jnp.maximum(band - 1, 0), 1 - slot)

    gram(BANDS - 1, 1)

    @pl.loop(0, VECS // 2)
    def _(block):
        for h in range(2):
            for i in range(2):
                parts[block % 2, block // 2, 4 * i : 4 * i + 4, COLS * h : COLS * (h + 1)] = scale * product[
                    h, pl.ds(2 * block + i, 4, stride=VECS), :
                ]

    swap = remote(parts.at[1 - core], arrived_core, core_send.at[0], core_recv.at[0], partner)
    swap.start()
    swap.wait()
    own[...] = parts[core] + arrived_core[...]

    moves = []
    for d, device in enumerate(in_wide):
        target = lax.rem(chip + wide_steps[d], chips)
        moves.append(remote(own.at[target], arrived_wide.at[d], wide_send.at[d], wide_recv.at[d], device))
    for move in moves:
        move.start()
    for move in moves:
        move.wait_recv()
    total = own[chip]
    for d in range(chips - 1):
        total = total + arrived_wide[d]
    whole[...] = total
    for move in moves:
        move.wait_send()

    moves = []
    for d, device in enumerate(in_narrow):
        moves.append(remote(whole, arrived_narrow.at[d], narrow_send.at[d], narrow_recv.at[d], device))
    for move in moves:
        move.start()
    for move in moves:
        move.wait_recv()
    total = whole[...]
    for d in range(narrow_size - 1):
        total = total + arrived_narrow[d]
    for b in range(OPS):
        turn = lax.rem(2 * COLS - VECS * (b % 2) - 8 * narrow, COLS)
        mine = pltpu.roll(total[:, COLS * (b // 2) : COLS * (b // 2 + 1)], turn, 1)
        for i in range(2):
            staged[i, pl.ds(b, OPS, stride=OPS), :] = mine[OPS * i : OPS * (i + 1)]
    for i in range(2):
        out_ref[i] = jnp.transpose(staged[i])[: VECS // narrow_size]
    for move in moves + moves_r + moves_l + moves_s:
        move.wait_send()


def on_device(left, right, bond_signs, hop):
    wide_size = lax.axis_size("wide")
    narrow_size = lax.axis_size("narrow")
    chips = wide_size // 2
    scale = 1.0 / math.sqrt(ROWS * COLS * wide_size * narrow_size)
    hbm = pl.BlockSpec(memory_space=pl.ANY)
    dma = pltpu.SemaphoreType.DMA
    block = (8, OPS * VECS)
    spread = pl.pallas_call(
        functools.partial(moments_kernel, scale, chips),
        out_shape=jax.ShapeDtypeStruct((2, VECS // narrow_size, OPS * OPS), F32),
        in_specs=[hbm] * 4,
        out_specs=pl.BlockSpec(memory_space=pltpu.VMEM),
        scratch_shapes=[
            pltpu.VMEM((VECS, ROWS, COLS), BF16),
            pltpu.VMEM((VECS, ROWS, COLS), BF16),
            pltpu.VMEM((OPS, 2 * RANGE, ROWS, COLS), jnp.int32),
            pltpu.SMEM((OPS, RANGE), F32),
            pltpu.VMEM((VECS * PITCH, COLS), F32),
            pltpu.VMEM((ROWS + 2 * RANGE, VECS, COLS), F32),
            pltpu.VMEM((ROWS + 2 * RANGE, VECS, COLS), F32),
            pltpu.VMEM((ROWS, VECS, COLS), BF16),
            pltpu.VMEM((ROWS, VECS, COLS), BF16),
            pltpu.VMEM((8 * OPS, ROWS + 16, COLS), F32),
            pltpu.VMEM((16, ROWS, COLS), F32),
            pltpu.VMEM((2 * COLS, 8 * COLS), BF16),
            pltpu.VMEM((RANGE, VECS, COLS), BF16),
            pltpu.VMEM((RANGE, VECS, COLS), BF16),
            pltpu.VMEM((2, RANGE * VECS, 8 * COLS), F32),
            pltpu.VMEM((BANDS, OPS * VECS, RANGE * COLS), BF16),
            pltpu.VMEM((2, OPS * VECS, RANGE * COLS), BF16),
            pltpu.VMEM((2, OPS * VECS, COLS), F32),
            pltpu.VMEM((2, 2, RANGE, VECS, COLS), BF16),
            pltpu.VMEM((2, 2, RANGE, VECS, COLS), BF16),
            pltpu.VMEM((2, 2, COLS // 2, 2 * COLS), BF16),
            pltpu.VMEM((2, 2, COLS // 2, 2 * COLS), BF16),
            pltpu.VMEM((2, 8 * RANGE, COLS), F32),
            pltpu.VMEM((2, 8 * RANGE, COLS), BF16),
            pltpu.VMEM((2, 8 * RANGE, COLS), BF16),
            pltpu.VMEM((2, ROWS, COLS), BF16),
            pltpu.VMEM((2, ROWS, COLS), BF16),
            pltpu.VMEM((2, chips) + block, F32),
            pltpu.VMEM((chips,) + block, F32),
            pltpu.VMEM((chips,) + block, F32),
            pltpu.VMEM((chips - 1,) + block, F32),
            pltpu.VMEM(block, F32),
            pltpu.VMEM((narrow_size - 1,) + block, F32),
            pltpu.VMEM((2, OPS * OPS, COLS), F32),
            dma((4,)),
            dma((3, 4)),
            dma((3, 4)),
            dma((1,)),
            dma((1,)),
            dma((chips - 1,)),
            dma((chips - 1,)),
            dma((narrow_size - 1,)),
            dma((narrow_size - 1,)),
        ],
        compiler_params=pltpu.CompilerParams(
            collective_id=0, has_side_effects=True, vmem_limit_bytes=60 << 20
        ),
        name="moments",
    )(left, right, bond_signs, hop)
    return spread.transpose(2, 0, 1)


def solution(mesh):
    in_specs = (
        P(None, "wide", "narrow"),
        P(None, "wide", "narrow"),
        P(None, None, "wide", "narrow"),
        P(),
    )
    return jax.shard_map(
        on_device, mesh=mesh, in_specs=in_specs, out_specs=P(None, "wide", "narrow"), check_vma=False
    )
```

```python
import functools
import math

import jax
import jax.numpy as jnp
from jax import lax
from jax.experimental import pallas as pl
from jax.experimental.pallas import tpu as pltpu
from jax.sharding import PartitionSpec as P

OPS = 4
RANGE = 4
VECS = 64
ROWS = 64
COLS = 128
PITCH = 72
BANDS = ROWS // RANGE
STEPS = (1, 2, 3, 4, -1, -2, -3, -4)
MESH = pl.DeviceIdType.MESH
F32 = jnp.float32
BF16 = jnp.bfloat16


def iota(shape, dim):
    return lax.broadcasted_iota(jnp.int32, shape, dim)


def ones_where(condition):
    return jnp.where(condition, 1.0, 0.0).astype(BF16)


def moments_kernel(
    chips, left_hbm, right_hbm, bits_hbm, hop_hbm, out_ref,
    left_ref, right_ref, bits_ref, hop_ref,
    flat, field_r, field_l, plain_r, plain_l, weight, weight_adj, shifter, packed_r, packed_l,
    slid, first, back, product,
    row_send, row_recv, col_send, col_recv, sr_stage, sr_send, sr_recv, sc_send, sc_recv,
    parts, own, arrived_core, arrived_wide, whole, arrived_narrow,
    staged, load_sem, send_sem, recv_sem, core_send, core_recv, wide_send, wide_recv, narrow_send, narrow_recv,
):
    loads = [
        pltpu.make_async_copy(source, target, load_sem.at[i])
        for i, (source, target) in enumerate(
            ((right_hbm, right_ref), (bits_hbm, bits_ref), (hop_hbm, hop_ref), (left_hbm, left_ref))
        )
    ]
    for load in loads:
        load.start()

    wide_size = lax.axis_size("wide")
    narrow_size = lax.axis_size("narrow")
    wide = lax.axis_index("wide")
    narrow = lax.axis_index("narrow")
    w_up, w_down = lax.rem(wide + 1, wide_size), lax.rem(wide + wide_size - 1, wide_size)
    n_up, n_down = lax.rem(narrow + 1, narrow_size), lax.rem(narrow + narrow_size - 1, narrow_size)
    sides = ((w_up, narrow), (w_down, narrow), (wide, n_up), (wide, n_down))
    core, chip = lax.rem(wide, 2), wide // 2
    partner = (wide + 1 - 2 * core, narrow)
    wide_steps = sorted(range(1, chips), key=lambda d: -min(d, chips - d))
    narrow_steps = sorted(range(1, narrow_size), key=lambda d: -min(d, narrow_size - d))
    in_wide = [(2 * lax.rem(chip + d, chips) + core, narrow) for d in wide_steps]
    in_narrow = [(wide, lax.rem(narrow + d, narrow_size)) for d in narrow_steps]

    barrier = pltpu.get_barrier_semaphore()
    everyone = [sides[0], sides[1]] + in_narrow[::-1] + in_wide[::-1]
    for device in everyone:
        pl.semaphore_signal(barrier, inc=1, device_id=device, device_id_type=MESH)

    def remote(source, target, sent, received, device):
        return pltpu.make_async_remote_copy(
            src_ref=source, dst_ref=target, send_sem=sent, recv_sem=received,
            device_id=device, device_id_type=MESH,
        )

    kappa = iota((2 * COLS, COLS), 0)
    tail = kappa - COLS
    edge = jnp.where(tail < COLS // 2, tail % RANGE - RANGE, tail % RANGE + COLS)
    origin = jnp.where(kappa < COLS, kappa, edge) - iota((2 * COLS, COLS), 1)
    for t, step in enumerate(STEPS):
        shifter[:, COLS * t : COLS * (t + 1)] = ones_where(origin == step)

    spot_row = iota((COLS, 2 * COLS), 0)
    spot_band = spot_row % (COLS // 2) // RANGE
    spot_col = spot_row % RANGE + jnp.where(spot_row < COLS // 2, COLS - RANGE, 0)
    spot_lane = COLS * spot_band + spot_col - iota((COLS, 2 * COLS), 1)

    def transposed(source, field, plain):
        @pl.loop(0, VECS, unroll=8)
        def _(v):
            flat[pl.ds(pl.multiple_of(v * PITCH, 8), ROWS), :] = source[v].astype(F32)

        @pl.loop(0, ROWS, unroll=8)
        def _(row):
            groups = [flat[pl.ds(8 * g * PITCH + row, 8, stride=PITCH), :] for g in range(VECS // 8)]
            whole_row = jnp.concatenate(groups, axis=0)
            field[row + RANGE] = whole_row
            plain[row] = whole_row.astype(BF16)

    def edges(side, plain):
        row_send[side, 0] = plain[ROWS - RANGE : ROWS]
        row_send[side, 1] = plain[0:RANGE]
        sums = [jnp.zeros((COLS, COLS), F32) for _ in range(2)]
        for c in range(BANDS // 2):
            pick = ones_where(spot_lane == 2 * COLS * c)
            bands = [
                plain[RANGE * b : RANGE * (b + 1)].reshape(RANGE * VECS, COLS)
                for b in (2 * c, 2 * c + 1)
            ]
            both = jnp.concatenate(bands, axis=1)
            for n in range(2):
                sums[n] = sums[n] + lax.dot_general(
                    pick, both[COLS * n : COLS * (n + 1)], (((1,), (1,)), ((), ())),
                    preferred_element_type=F32,
                )
        picked = jnp.concatenate(sums, axis=1)
        col_send[side, 0] = picked[: COLS // 2].astype(BF16)
        col_send[side, 1] = picked[COLS // 2 :].astype(BF16)

    def copies(slot, row_pair, col_pair):
        made = []
        for way in range(4):
            (source, target), part = (row_pair, way) if way < 2 else (col_pair, way - 2)
            made.append(
                remote(
                    source.at[part], target.at[part], send_sem.at[slot, way], recv_sem.at[slot, way],
                    sides[way],
                )
            )
        return made

    def landed(side, field, packed, moves):
        for move in moves:
            move.wait_recv()
        field[0:RANGE] = row_recv[side, 0].astype(F32)
        field[ROWS + RANGE : ROWS + 2 * RANGE] = row_recv[side, 1].astype(F32)
        strips = jnp.concatenate([col_recv[side, way].astype(F32) for way in range(2)], axis=0)
        packed[...] = jnp.transpose(strips).astype(BF16).reshape(RANGE, VECS, COLS)

    loads[0].wait()
    transposed(right_ref, field_r, plain_r)
    edges(0, plain_r)
    pl.semaphore_wait(barrier, len(everyone))
    moves_r = copies(0, (row_send.at[0], row_recv.at[0]), (col_send.at[0], col_recv.at[0]))
    for move in moves_r:
        move.start()

    loads[3].wait()
    transposed(left_ref, field_l, plain_l)
    edges(1, plain_l)
    moves_l = copies(1, (row_send.at[1], row_recv.at[1]), (col_send.at[1], col_recv.at[1]))
    for move in moves_l:
        move.start()

    loads[1].wait()
    loads[2].wait()

    def coefficient(op, tap):
        return hop_ref[op, tap % RANGE] * (1.0 if tap < RANGE else -1.0)

    def sign_of(op, tap):
        return (2 * bits_ref[op, tap] - 1).astype(F32)

    small = iota((ROWS, COLS), 1)
    for half, op in enumerate((0, 2)):
        for tap in range(2 * RANGE):
            sign = sign_of(op, tap)
            weight[8 * op + tap, 8 : 8 + ROWS, :] = coefficient(op, tap) * sign
            way, at = (0, ROWS - RANGE) if tap < RANGE else (1, 0)
            spot = (4 * half + tap % RANGE) * RANGE
            sr_stage[way, spot : spot + RANGE, :] = sign[at : at + RANGE]
    for way in range(2):
        sr_send[way] = sr_stage[way].astype(BF16)
    for way in range(2):
        held = jnp.zeros((ROWS, COLS), F32)
        for half, op in enumerate((1, 3)):
            for k in range(RANGE):
                tap = RANGE * way + k
                sign = sign_of(op, tap)
                weight[8 * op + tap, 8 : 8 + ROWS, :] = coefficient(op, tap) * sign
                at = COLS // 2 * way + RANGE * (4 * half + k)
                moved = pltpu.roll(sign, at + RANGE if way == 0 else at, 1) if at or way == 0 else sign
                held = jnp.where(small // RANGE == at // RANGE, moved, held)
        sc_send[way] = held.astype(BF16)
    moves_s = copies(2, (sr_send, sr_recv), (sc_send, sc_recv))
    for move in moves_s:
        move.start()

    def along_rows(field, row, adjoint):
        sums = [None, None]
        for tap in range(2 * RANGE):
            step = -STEPS[tap] if adjoint else STEPS[tap]
            x = field[RANGE + row + step]
            for half, op in enumerate((0, 2)):
                at = 8 + row + (step if adjoint else 0)
                term = weight[8 * op + tap, pl.ds(at, 1), :] * x
                sums[half] = term if sums[half] is None else sums[half] + term
        return sums

    wide_lane = iota((VECS, COLS), 1) % (COLS // 2) // RANGE

    def shift_cols(plain, packed, band, slot):
        inside = wide_lane == band
        rows = []
        for j in range(RANGE):
            strip = packed[j]
            rows.append(
                jnp.concatenate([plain[RANGE * band + j], jnp.where(inside, strip, jnp.zeros_like(strip))], axis=1)
            )
        lhs = jnp.concatenate(rows, axis=0)
        for t in range(4):
            at = slice(2 * COLS * t, 2 * COLS * (t + 1))
            slid[slot, :, at] = jnp.dot(lhs, shifter[:, at], preferred_element_type=F32)

    def along_cols(slot, j, row, adjoint):
        sums = [None, None]
        for t in range(2 * RANGE):
            tap = (t + RANGE) % (2 * RANGE) if adjoint else t
            x = slid[slot, VECS * j : VECS * (j + 1), COLS * t : COLS * (t + 1)]
            for half, op in enumerate((1, 3)):
                if adjoint:
                    w = weight_adj[8 * half + tap, pl.ds(row, 1), :]
                else:
                    w = weight[8 * op + tap, pl.ds(8 + row, 1), :]
                term = w * x
                sums[half] = term if sums[half] is None else sums[half] + term
        return sums

    def applied(field, band, slot, adjoint, store):
        for j in range(RANGE):
            row = RANGE * band + j
            even = along_rows(field, row, adjoint)
            odd = along_cols(slot, j, row, adjoint)
            for op in range(OPS):
                value = (odd if op % 2 else even)[op // 2]
                store(slice(VECS * op, VECS * (op + 1)), slice(COLS * j, COLS * (j + 1)), value.astype(BF16))

    def row_ops(band):
        for j in range(RANGE):
            sums = along_rows(field_r, RANGE * band + j, False)
            for half, op in enumerate((0, 2)):
                first[band, VECS * op : VECS * (op + 1), COLS * j : COLS * (j + 1)] = sums[half].astype(BF16)

    def col_ops(band, slot):
        for j in range(RANGE):
            sums = along_cols(slot, j, RANGE * band + j, False)
            for half, op in enumerate((1, 3)):
                first[band, VECS * op : VECS * (op + 1), COLS * j : COLS * (j + 1)] = sums[half].astype(BF16)

    @pl.loop(1, BANDS - 1)
    def _(band):
        row_ops(band)

    landed(0, field_r, packed_r, moves_r)
    shift_cols(plain_r, packed_r, 0, 0)
    for band in (0, BANDS - 1):
        row_ops(band)

    @pl.loop(0, BANDS // 2)
    def _(couple):
        for slot in range(2):
            band = 2 * couple + slot
            col_ops(band, slot)
            shift_cols(plain_r, packed_r, jnp.minimum(band + 1, BANDS - 1), 1 - slot)

    for move in moves_s:
        move.wait_recv()
    landed(1, field_l, packed_l, moves_l)

    for way in range(2):
        sr_stage[way] = sr_recv[way].astype(F32)
    for half, op in enumerate((0, 2)):
        for tap in range(2 * RANGE):
            way, at = (0, 8 - RANGE) if tap < RANGE else (1, 8 + ROWS)
            spot = (4 * half + tap % RANGE) * RANGE
            weight[8 * op + tap, at : at + RANGE, :] = coefficient(op, tap) * sr_stage[way, spot : spot + RANGE, :]
    strips = sc_recv[0].astype(F32) + sc_recv[1].astype(F32)
    for tap in range(2 * RANGE):
        lhs = []
        for half, op in enumerate((1, 3)):
            spot = 4 * half + tap % RANGE
            inside = small % (COLS // 2) // RANGE == spot
            lhs.append(jnp.concatenate([sign_of(op, tap), jnp.where(inside, strips, 0.0)], axis=1))
        t = (tap + RANGE) % (2 * RANGE)
        moved = jnp.dot(
            jnp.concatenate(lhs, axis=0).astype(BF16), shifter[:, COLS * t : COLS * (t + 1)],
            preferred_element_type=F32,
        )
        for half, op in enumerate((1, 3)):
            weight_adj[8 * half + tap] = coefficient(op, tap) * moved[ROWS * half : ROWS * (half + 1)]

    product[...] = jnp.zeros_like(product)
    back[...] = jnp.zeros_like(back)

    def gram(band, slot):
        part = lax.dot_general(back[slot], first[band], (((1,), (1,)), ((), ())), preferred_element_type=F32)
        for h in range(2):
            product[h] += part[:, COLS * h : COLS * (h + 1)]

    shift_cols(plain_l, packed_l, 0, 0)

    @pl.loop(0, BANDS // 2)
    def _(couple):
        for slot in range(2):
            band = 2 * couple + slot

            def store(vecs, cols, value):
                back[slot, vecs, cols] = value

            applied(field_l, band, slot, True, store)
            shift_cols(plain_l, packed_l, jnp.minimum(band + 1, BANDS - 1), 1 - slot)
            gram(jnp.maximum(band - 1, 0), 1 - slot)

    gram(BANDS - 1, 1)

    def collect(side):
        @pl.loop(0, chips, unroll=4)
        def _(place):
            for h in range(2):
                for i in range(2):
                    parts[side, place, 4 * i : 4 * i + 4, COLS * h : COLS * (h + 1)] = product[
                        h, pl.ds(4 * place + 2 * side + i, 4, stride=VECS), :
                    ]

    collect(1 - core)
    swap = remote(parts.at[1 - core], arrived_core, core_send.at[0], core_recv.at[0], partner)
    swap.start()
    collect(core)
    swap.wait()
    own[...] = parts[core] + arrived_core[...]

    moves = []
    for d, device in enumerate(in_wide):
        target = lax.rem(chip + wide_steps[d], chips)
        moves.append(remote(own.at[target], arrived_wide.at[d], wide_send.at[d], wide_recv.at[d], device))
    for move in moves:
        move.start()
    for move in moves:
        move.wait_recv()
    total = own[chip]
    for d in range(chips - 1):
        total = total + arrived_wide[d]
    whole[...] = total
    for move in moves:
        move.wait_send()

    moves = []
    for d, device in enumerate(in_narrow):
        moves.append(remote(whole, arrived_narrow.at[d], narrow_send.at[d], narrow_recv.at[d], device))
    for move in moves:
        move.start()
    for move in moves:
        move.wait_recv()
    total = whole[...]
    for d in range(narrow_size - 1):
        total = total + arrived_narrow[d]
    for b in range(OPS):
        turn = lax.rem(2 * COLS - VECS * (b % 2) - 8 * narrow, COLS)
        mine = pltpu.roll(total[:, COLS * (b // 2) : COLS * (b // 2 + 1)], turn, 1)
        for i in range(2):
            staged[i, pl.ds(b, OPS, stride=OPS), :] = mine[OPS * i : OPS * (i + 1)]
    for i in range(2):
        out_ref[i] = jnp.transpose(staged[i])[: VECS // narrow_size]
    for move in moves + moves_r + moves_l + moves_s:
        move.wait_send()


def on_device(left, right, bond_signs, hop):
    wide_size = lax.axis_size("wide")
    narrow_size = lax.axis_size("narrow")
    chips = wide_size // 2
    scale = 1.0 / math.sqrt(ROWS * COLS * wide_size * narrow_size)
    hbm = pl.BlockSpec(memory_space=pl.ANY)
    dma = pltpu.SemaphoreType.DMA
    block = (8, OPS * VECS)
    spread = pl.pallas_call(
        functools.partial(moments_kernel, chips),
        out_shape=jax.ShapeDtypeStruct((2, VECS // narrow_size, OPS * OPS), F32),
        in_specs=[hbm] * 4,
        out_specs=pl.BlockSpec(memory_space=pltpu.VMEM),
        scratch_shapes=[
            pltpu.VMEM((VECS, ROWS, COLS), BF16),
            pltpu.VMEM((VECS, ROWS, COLS), BF16),
            pltpu.VMEM((OPS, 2 * RANGE, ROWS, COLS), jnp.int32),
            pltpu.SMEM((OPS, RANGE), F32),
            pltpu.VMEM((VECS * PITCH, COLS), F32),
            pltpu.VMEM((ROWS + 2 * RANGE, VECS, COLS), F32),
            pltpu.VMEM((ROWS + 2 * RANGE, VECS, COLS), F32),
            pltpu.VMEM((ROWS, VECS, COLS), BF16),
            pltpu.VMEM((ROWS, VECS, COLS), BF16),
            pltpu.VMEM((8 * OPS, ROWS + 16, COLS), F32),
            pltpu.VMEM((16, ROWS, COLS), F32),
            pltpu.VMEM((2 * COLS, 8 * COLS), BF16),
            pltpu.VMEM((RANGE, VECS, COLS), BF16),
            pltpu.VMEM((RANGE, VECS, COLS), BF16),
            pltpu.VMEM((2, RANGE * VECS, 8 * COLS), F32),
            pltpu.VMEM((BANDS, OPS * VECS, RANGE * COLS), BF16),
            pltpu.VMEM((2, OPS * VECS, RANGE * COLS), BF16),
            pltpu.VMEM((2, OPS * VECS, COLS), F32),
            pltpu.VMEM((2, 2, RANGE, VECS, COLS), BF16),
            pltpu.VMEM((2, 2, RANGE, VECS, COLS), BF16),
            pltpu.VMEM((2, 2, COLS // 2, 2 * COLS), BF16),
            pltpu.VMEM((2, 2, COLS // 2, 2 * COLS), BF16),
            pltpu.VMEM((2, 8 * RANGE, COLS), F32),
            pltpu.VMEM((2, 8 * RANGE, COLS), BF16),
            pltpu.VMEM((2, 8 * RANGE, COLS), BF16),
            pltpu.VMEM((2, ROWS, COLS), BF16),
            pltpu.VMEM((2, ROWS, COLS), BF16),
            pltpu.VMEM((2, chips) + block, F32),
            pltpu.VMEM((chips,) + block, F32),
            pltpu.VMEM((chips,) + block, F32),
            pltpu.VMEM((chips - 1,) + block, F32),
            pltpu.VMEM(block, F32),
            pltpu.VMEM((narrow_size - 1,) + block, F32),
            pltpu.VMEM((2, OPS * OPS, COLS), F32),
            dma((4,)),
            dma((3, 4)),
            dma((3, 4)),
            dma((1,)),
            dma((1,)),
            dma((chips - 1,)),
            dma((chips - 1,)),
            dma((narrow_size - 1,)),
            dma((narrow_size - 1,)),
        ],
        compiler_params=pltpu.CompilerParams(
            collective_id=0, has_side_effects=True, vmem_limit_bytes=60 << 20
        ),
        name="moments",
    )(left, right, bond_signs, hop)
    return spread.transpose(2, 0, 1) * F32(scale)


def solution(mesh):
    in_specs = (
        P(None, "wide", "narrow"),
        P(None, "wide", "narrow"),
        P(None, None, "wide", "narrow"),
        P(),
    )
    return jax.shard_map(
        on_device, mesh=mesh, in_specs=in_specs, out_specs=P(None, "wide", "narrow"), check_vma=False
    )
```

```python
import functools
import math

import jax
import jax.numpy as jnp
from jax import lax
from jax.experimental import pallas as pl
from jax.experimental.pallas import tpu as pltpu
from jax.sharding import PartitionSpec as P

OPS = 4
RANGE = 4
VECS = 64
ROWS = 64
COLS = 128
PITCH = 72
BANDS = ROWS // RANGE
STEPS = (1, 2, 3, 4, -1, -2, -3, -4)
MESH = pl.DeviceIdType.MESH
F32 = jnp.float32
BF16 = jnp.bfloat16


def iota(shape, dim):
    return lax.broadcasted_iota(jnp.int32, shape, dim)


def ones_where(condition):
    return jnp.where(condition, 1.0, 0.0).astype(BF16)


def moments_kernel(
    chips, left_hbm, right_hbm, bits_hbm, hop_hbm, out_ref,
    left_ref, right_ref, bits_ref, hop_ref,
    flat, field_r, field_l, plain_r, plain_l, weight, weight_adj, shifter, packed_r, packed_l,
    slid, first, back, product,
    row_send, row_recv, col_send, col_recv, sr_stage, sr_send, sr_recv, sc_send, sc_recv,
    parts, own, arrived_core, arrived_wide, whole, arrived_narrow,
    staged, load_sem, send_sem, recv_sem, core_send, core_recv, wide_send, wide_recv, narrow_send, narrow_recv,
):
    quarters = [pl.ds(VECS // 4 * q, VECS // 4) for q in range(4)]
    loads = [
        pltpu.make_async_copy(source, target, load_sem.at[i])
        for i, (source, target) in enumerate(
            tuple((right_hbm.at[q], right_ref.at[q]) for q in quarters)
            + ((left_hbm, left_ref), (bits_hbm, bits_ref), (hop_hbm, hop_ref))
        )
    ]
    for load in loads:
        load.start()

    wide_size = lax.axis_size("wide")
    narrow_size = lax.axis_size("narrow")
    wide = lax.axis_index("wide")
    narrow = lax.axis_index("narrow")
    w_up, w_down = lax.rem(wide + 1, wide_size), lax.rem(wide + wide_size - 1, wide_size)
    n_up, n_down = lax.rem(narrow + 1, narrow_size), lax.rem(narrow + narrow_size - 1, narrow_size)
    sides = ((w_up, narrow), (w_down, narrow), (wide, n_up), (wide, n_down))
    core, chip = lax.rem(wide, 2), wide // 2
    partner = (wide + 1 - 2 * core, narrow)
    wide_steps = sorted(range(1, chips), key=lambda d: -min(d, chips - d))
    narrow_steps = sorted(range(1, narrow_size), key=lambda d: -min(d, narrow_size - d))
    in_wide = [(2 * lax.rem(chip + d, chips) + core, narrow) for d in wide_steps]
    in_narrow = [(wide, lax.rem(narrow + d, narrow_size)) for d in narrow_steps]

    barrier = pltpu.get_barrier_semaphore()
    everyone = [sides[0], sides[1]] + in_narrow[::-1] + in_wide[::-1]
    for device in everyone:
        pl.semaphore_signal(barrier, inc=1, device_id=device, device_id_type=MESH)

    def remote(source, target, sent, received, device):
        return pltpu.make_async_remote_copy(
            src_ref=source, dst_ref=target, send_sem=sent, recv_sem=received,
            device_id=device, device_id_type=MESH,
        )

    kappa = iota((2 * COLS, COLS), 0)
    tail = kappa - COLS
    edge = jnp.where(tail < COLS // 2, tail % RANGE - RANGE, tail % RANGE + COLS)
    origin = jnp.where(kappa < COLS, kappa, edge) - iota((2 * COLS, COLS), 1)
    for t, step in enumerate(STEPS):
        shifter[:, COLS * t : COLS * (t + 1)] = ones_where(origin == step)

    spot_row = iota((COLS, 2 * COLS), 0)
    spot_band = spot_row % (COLS // 2) // RANGE
    spot_col = spot_row % RANGE + jnp.where(spot_row < COLS // 2, COLS - RANGE, 0)
    spot_lane = COLS * spot_band + spot_col - iota((COLS, 2 * COLS), 1)

    def transposed(source, field, plain, arrivals):
        count = VECS // len(arrivals)
        for part, arrival in enumerate(arrivals):
            arrival.wait()

            @pl.loop(count * part, count * (part + 1), unroll=8)
            def _(v):
                flat[pl.ds(pl.multiple_of(v * PITCH, 8), ROWS), :] = source[v].astype(F32)

        @pl.loop(0, ROWS, unroll=8)
        def _(row):
            groups = [flat[pl.ds(8 * g * PITCH + row, 8, stride=PITCH), :] for g in range(VECS // 8)]
            whole_row = jnp.concatenate(groups, axis=0)
            field[row + RANGE] = whole_row
            plain[row] = whole_row.astype(BF16)

    def edges(side, plain):
        row_send[side, 0] = plain[ROWS - RANGE : ROWS]
        row_send[side, 1] = plain[0:RANGE]
        sums = [jnp.zeros((COLS, COLS), F32) for _ in range(2)]
        for c in range(BANDS // 2):
            pick = ones_where(spot_lane == 2 * COLS * c)
            bands = [
                plain[RANGE * b : RANGE * (b + 1)].reshape(RANGE * VECS, COLS)
                for b in (2 * c, 2 * c + 1)
            ]
            both = jnp.concatenate(bands, axis=1)
            for n in range(2):
                sums[n] = sums[n] + lax.dot_general(
                    pick, both[COLS * n : COLS * (n + 1)], (((1,), (1,)), ((), ())),
                    preferred_element_type=F32,
                )
        picked = jnp.concatenate(sums, axis=1)
        col_send[side, 0] = picked[: COLS // 2].astype(BF16)
        col_send[side, 1] = picked[COLS // 2 :].astype(BF16)

    def copies(slot, row_pair, col_pair):
        made = []
        for way in range(4):
            (source, target), part = (row_pair, way) if way < 2 else (col_pair, way - 2)
            made.append(
                remote(
                    source.at[part], target.at[part], send_sem.at[slot, way], recv_sem.at[slot, way],
                    sides[way],
                )
            )
        return made

    def landed(side, field, packed, moves):
        for move in moves:
            move.wait_recv()
        field[0:RANGE] = row_recv[side, 0].astype(F32)
        field[ROWS + RANGE : ROWS + 2 * RANGE] = row_recv[side, 1].astype(F32)
        strips = jnp.concatenate([col_recv[side, way].astype(F32) for way in range(2)], axis=0)
        packed[...] = jnp.transpose(strips).astype(BF16).reshape(RANGE, VECS, COLS)

    product[...] = jnp.zeros_like(product)
    back[1] = jnp.zeros_like(back[1])

    transposed(right_ref, field_r, plain_r, loads[:4])
    edges(0, plain_r)
    pl.semaphore_wait(barrier, len(everyone))
    moves_r = copies(0, (row_send.at[0], row_recv.at[0]), (col_send.at[0], col_recv.at[0]))
    for move in moves_r:
        move.start()

    transposed(left_ref, field_l, plain_l, loads[4:5])
    edges(1, plain_l)
    moves_l = copies(1, (row_send.at[1], row_recv.at[1]), (col_send.at[1], col_recv.at[1]))
    for move in moves_l:
        move.start()

    loads[5].wait()
    loads[6].wait()

    def coefficient(op, tap):
        return hop_ref[op, tap % RANGE] * (1.0 if tap < RANGE else -1.0)

    def sign_of(op, tap):
        return (2 * bits_ref[op, tap] - 1).astype(F32)

    small = iota((ROWS, COLS), 1)
    for half, op in enumerate((0, 2)):
        for tap in range(2 * RANGE):
            sign = sign_of(op, tap)
            weight[8 * op + tap, 8 : 8 + ROWS, :] = coefficient(op, tap) * sign
            way, at = (0, ROWS - RANGE) if tap < RANGE else (1, 0)
            spot = (4 * half + tap % RANGE) * RANGE
            sr_stage[way, spot : spot + RANGE, :] = sign[at : at + RANGE]
    for way in range(2):
        sr_send[way] = sr_stage[way].astype(BF16)
    for way in range(2):
        held = jnp.zeros((ROWS, COLS), F32)
        for half, op in enumerate((1, 3)):
            for k in range(RANGE):
                tap = RANGE * way + k
                sign = sign_of(op, tap)
                weight[8 * op + tap, 8 : 8 + ROWS, :] = coefficient(op, tap) * sign
                at = COLS // 2 * way + RANGE * (4 * half + k)
                moved = pltpu.roll(sign, at + RANGE if way == 0 else at, 1) if at or way == 0 else sign
                held = jnp.where(small // RANGE == at // RANGE, moved, held)
        sc_send[way] = held.astype(BF16)
    moves_s = copies(2, (sr_send, sr_recv), (sc_send, sc_recv))
    for move in moves_s:
        move.start()

    def along_rows(field, row, adjoint):
        sums = [None, None]
        for tap in range(2 * RANGE):
            step = -STEPS[tap] if adjoint else STEPS[tap]
            x = field[RANGE + row + step]
            for half, op in enumerate((0, 2)):
                at = 8 + row + (step if adjoint else 0)
                term = weight[8 * op + tap, pl.ds(at, 1), :] * x
                sums[half] = term if sums[half] is None else sums[half] + term
        return sums

    wide_lane = iota((VECS, COLS), 1) % (COLS // 2) // RANGE

    def shift_cols(plain, packed, band, slot):
        inside = wide_lane == band
        rows = []
        for j in range(RANGE):
            strip = packed[j]
            rows.append(
                jnp.concatenate([plain[RANGE * band + j], jnp.where(inside, strip, jnp.zeros_like(strip))], axis=1)
            )
        lhs = jnp.concatenate(rows, axis=0)
        for t in range(4):
            at = slice(2 * COLS * t, 2 * COLS * (t + 1))
            slid[slot, :, at] = jnp.dot(lhs, shifter[:, at], preferred_element_type=F32)

    def along_cols(slot, j, row, adjoint):
        sums = [None, None]
        for t in range(2 * RANGE):
            tap = (t + RANGE) % (2 * RANGE) if adjoint else t
            x = slid[slot, VECS * j : VECS * (j + 1), COLS * t : COLS * (t + 1)]
            for half, op in enumerate((1, 3)):
                if adjoint:
                    w = weight_adj[8 * half + tap, pl.ds(row, 1), :]
                else:
                    w = weight[8 * op + tap, pl.ds(8 + row, 1), :]
                term = w * x
                sums[half] = term if sums[half] is None else sums[half] + term
        return sums

    def applied(field, band, slot, adjoint, store):
        for j in range(RANGE):
            row = RANGE * band + j
            even = along_rows(field, row, adjoint)
            odd = along_cols(slot, j, row, adjoint)
            for op in range(OPS):
                value = (odd if op % 2 else even)[op // 2]
                store(slice(VECS * op, VECS * (op + 1)), slice(COLS * j, COLS * (j + 1)), value.astype(BF16))

    def row_ops(band):
        for j in range(RANGE):
            sums = along_rows(field_r, RANGE * band + j, False)
            for half, op in enumerate((0, 2)):
                first[band, VECS * op : VECS * (op + 1), COLS * j : COLS * (j + 1)] = sums[half].astype(BF16)

    def col_ops(band, slot):
        for j in range(RANGE):
            sums = along_cols(slot, j, RANGE * band + j, False)
            for half, op in enumerate((1, 3)):
                first[band, VECS * op : VECS * (op + 1), COLS * j : COLS * (j + 1)] = sums[half].astype(BF16)

    @pl.loop(1, BANDS - 1)
    def _(band):
        row_ops(band)

    landed(0, field_r, packed_r, moves_r)
    shift_cols(plain_r, packed_r, 0, 0)
    for band in (0, BANDS - 1):
        row_ops(band)

    @pl.loop(0, BANDS // 2)
    def _(couple):
        for slot in range(2):
            band = 2 * couple + slot
            col_ops(band, slot)
            shift_cols(plain_r, packed_r, jnp.minimum(band + 1, BANDS - 1), 1 - slot)

    for move in moves_s:
        move.wait_recv()
    landed(1, field_l, packed_l, moves_l)

    for way in range(2):
        sr_stage[way] = sr_recv[way].astype(F32)
    for half, op in enumerate((0, 2)):
        for tap in range(2 * RANGE):
            way, at = (0, 8 - RANGE) if tap < RANGE else (1, 8 + ROWS)
            spot = (4 * half + tap % RANGE) * RANGE
            weight[8 * op + tap, at : at + RANGE, :] = coefficient(op, tap) * sr_stage[way, spot : spot + RANGE, :]
    strips = sc_recv[0].astype(F32) + sc_recv[1].astype(F32)
    for tap in range(2 * RANGE):
        lhs = []
        for half, op in enumerate((1, 3)):
            spot = 4 * half + tap % RANGE
            inside = small % (COLS // 2) // RANGE == spot
            lhs.append(jnp.concatenate([sign_of(op, tap), jnp.where(inside, strips, 0.0)], axis=1))
        t = (tap + RANGE) % (2 * RANGE)
        moved = jnp.dot(
            jnp.concatenate(lhs, axis=0).astype(BF16), shifter[:, COLS * t : COLS * (t + 1)],
            preferred_element_type=F32,
        )
        for half, op in enumerate((1, 3)):
            weight_adj[8 * half + tap] = coefficient(op, tap) * moved[ROWS * half : ROWS * (half + 1)]

    def gram(band, slot):
        part = lax.dot_general(back[slot], first[band], (((1,), (1,)), ((), ())), preferred_element_type=F32)
        for h in range(2):
            product[h] += part[:, COLS * h : COLS * (h + 1)]

    shift_cols(plain_l, packed_l, 0, 0)

    @pl.loop(0, BANDS // 2)
    def _(couple):
        for slot in range(2):
            band = 2 * couple + slot

            def store(vecs, cols, value):
                back[slot, vecs, cols] = value

            applied(field_l, band, slot, True, store)
            shift_cols(plain_l, packed_l, jnp.minimum(band + 1, BANDS - 1), 1 - slot)
            gram(jnp.maximum(band - 1, 0), 1 - slot)

    gram(BANDS - 1, 1)

    def collect(side):
        @pl.loop(0, chips, unroll=4)
        def _(place):
            for h in range(2):
                for i in range(2):
                    parts[side, place, 4 * i : 4 * i + 4, COLS * h : COLS * (h + 1)] = product[
                        h, pl.ds(4 * place + 2 * side + i, 4, stride=VECS), :
                    ]

    collect(1 - core)
    swap = remote(parts.at[1 - core], arrived_core, core_send.at[0], core_recv.at[0], partner)
    swap.start()
    collect(core)
    swap.wait()
    own[...] = parts[core] + arrived_core[...]

    moves = []
    for d, device in enumerate(in_wide):
        target = lax.rem(chip + wide_steps[d], chips)
        moves.append(remote(own.at[target], arrived_wide.at[d], wide_send.at[d], wide_recv.at[d], device))
    for move in moves:
        move.start()
    for move in moves:
        move.wait_recv()
    total = own[chip]
    for d in range(chips - 1):
        total = total + arrived_wide[d]
    whole[...] = total

    sent = moves_r + moves_l + moves_s + moves
    moves = []
    for d, device in enumerate(in_narrow):
        moves.append(remote(whole, arrived_narrow.at[d], narrow_send.at[d], narrow_recv.at[d], device))
    for move in moves:
        move.start()
    for move in sent:
        move.wait_send()
    for move in moves:
        move.wait_recv()
    total = whole[...]
    for d in range(narrow_size - 1):
        total = total + arrived_narrow[d]
    for b in range(OPS):
        turn = lax.rem(2 * COLS - VECS * (b % 2) - 8 * narrow, COLS)
        mine = pltpu.roll(total[:, COLS * (b // 2) : COLS * (b // 2 + 1)], turn, 1)
        for i in range(2):
            staged[i, pl.ds(b, OPS, stride=OPS), :] = mine[OPS * i : OPS * (i + 1)]
    for i in range(2):
        out_ref[i] = jnp.transpose(staged[i])[: VECS // narrow_size]
    for move in moves:
        move.wait_send()


def on_device(left, right, bond_signs, hop):
    wide_size = lax.axis_size("wide")
    narrow_size = lax.axis_size("narrow")
    chips = wide_size // 2
    scale = 1.0 / math.sqrt(ROWS * COLS * wide_size * narrow_size)
    hbm = pl.BlockSpec(memory_space=pl.ANY)
    dma = pltpu.SemaphoreType.DMA
    block = (8, OPS * VECS)
    spread = pl.pallas_call(
        functools.partial(moments_kernel, chips),
        out_shape=jax.ShapeDtypeStruct((2, VECS // narrow_size, OPS * OPS), F32),
        in_specs=[hbm] * 4,
        out_specs=pl.BlockSpec(memory_space=pltpu.VMEM),
        scratch_shapes=[
            pltpu.VMEM((VECS, ROWS, COLS), BF16),
            pltpu.VMEM((VECS, ROWS, COLS), BF16),
            pltpu.VMEM((OPS, 2 * RANGE, ROWS, COLS), jnp.int32),
            pltpu.SMEM((OPS, RANGE), F32),
            pltpu.VMEM((VECS * PITCH, COLS), F32),
            pltpu.VMEM((ROWS + 2 * RANGE, VECS, COLS), F32),
            pltpu.VMEM((ROWS + 2 * RANGE, VECS, COLS), F32),
            pltpu.VMEM((ROWS, VECS, COLS), BF16),
            pltpu.VMEM((ROWS, VECS, COLS), BF16),
            pltpu.VMEM((8 * OPS, ROWS + 16, COLS), F32),
            pltpu.VMEM((16, ROWS, COLS), F32),
            pltpu.VMEM((2 * COLS, 8 * COLS), BF16),
            pltpu.VMEM((RANGE, VECS, COLS), BF16),
            pltpu.VMEM((RANGE, VECS, COLS), BF16),
            pltpu.VMEM((2, RANGE * VECS, 8 * COLS), F32),
            pltpu.VMEM((BANDS, OPS * VECS, RANGE * COLS), BF16),
            pltpu.VMEM((2, OPS * VECS, RANGE * COLS), BF16),
            pltpu.VMEM((2, OPS * VECS, COLS), F32),
            pltpu.VMEM((2, 2, RANGE, VECS, COLS), BF16),
            pltpu.VMEM((2, 2, RANGE, VECS, COLS), BF16),
            pltpu.VMEM((2, 2, COLS // 2, 2 * COLS), BF16),
            pltpu.VMEM((2, 2, COLS // 2, 2 * COLS), BF16),
            pltpu.VMEM((2, 8 * RANGE, COLS), F32),
            pltpu.VMEM((2, 8 * RANGE, COLS), BF16),
            pltpu.VMEM((2, 8 * RANGE, COLS), BF16),
            pltpu.VMEM((2, ROWS, COLS), BF16),
            pltpu.VMEM((2, ROWS, COLS), BF16),
            pltpu.VMEM((2, chips) + block, F32),
            pltpu.VMEM((chips,) + block, F32),
            pltpu.VMEM((chips,) + block, F32),
            pltpu.VMEM((chips - 1,) + block, F32),
            pltpu.VMEM(block, F32),
            pltpu.VMEM((narrow_size - 1,) + block, F32),
            pltpu.VMEM((2, OPS * OPS, COLS), F32),
            dma((7,)),
            dma((3, 4)),
            dma((3, 4)),
            dma((1,)),
            dma((1,)),
            dma((chips - 1,)),
            dma((chips - 1,)),
            dma((narrow_size - 1,)),
            dma((narrow_size - 1,)),
        ],
        compiler_params=pltpu.CompilerParams(
            collective_id=0, has_side_effects=True, vmem_limit_bytes=60 << 20
        ),
        name="moments",
    )(left, right, bond_signs, hop)
    return spread.transpose(2, 0, 1) * F32(scale)


def solution(mesh):
    in_specs = (
        P(None, "wide", "narrow"),
        P(None, "wide", "narrow"),
        P(None, None, "wide", "narrow"),
        P(),
    )
    return jax.shard_map(
        on_device, mesh=mesh, in_specs=in_specs, out_specs=P(None, "wide", "narrow"), check_vma=False
    )
```

```python
import functools
import math

import jax
import jax.numpy as jnp
from jax import lax
from jax.experimental import pallas as pl
from jax.experimental.pallas import tpu as pltpu
from jax.sharding import PartitionSpec as P

OPS = 4
RANGE = 4
VECS = 64
ROWS = 64
COLS = 128
PITCH = 72
BANDS = ROWS // RANGE
STEPS = (1, 2, 3, 4, -1, -2, -3, -4)
MESH = pl.DeviceIdType.MESH
F32 = jnp.float32
BF16 = jnp.bfloat16


def iota(shape, dim):
    return lax.broadcasted_iota(jnp.int32, shape, dim)


def ones_where(condition):
    return jnp.where(condition, 1.0, 0.0).astype(BF16)


def moments_kernel(
    chips, left_hbm, right_hbm, bits_hbm, hop_hbm, out_ref,
    left_ref, right_ref, bits_ref, hop_ref,
    flat, field_r, field_l, plain_r, plain_l, weight, weight_adj, shifter, packed_r, packed_l,
    slid, first, back, product,
    row_send, row_recv, col_send, col_recv, sr_stage, sr_send, sr_recv, sc_send, sc_recv,
    parts, own, arrived_core, arrived_wide, whole, arrived_narrow,
    staged, load_sem, send_sem, recv_sem, core_send, core_recv, wide_send, wide_recv, narrow_send, narrow_recv,
):
    quarters = [pl.ds(VECS // 4 * q, VECS // 4) for q in range(4)]
    loads = [
        pltpu.make_async_copy(source, target, load_sem.at[i])
        for i, (source, target) in enumerate(
            tuple((right_hbm.at[q], right_ref.at[q]) for q in quarters)
            + ((left_hbm, left_ref), (bits_hbm, bits_ref), (hop_hbm, hop_ref))
        )
    ]
    for load in loads:
        load.start()

    wide_size = lax.axis_size("wide")
    narrow_size = lax.axis_size("narrow")
    wide = lax.axis_index("wide")
    narrow = lax.axis_index("narrow")
    w_up, w_down = lax.rem(wide + 1, wide_size), lax.rem(wide + wide_size - 1, wide_size)
    n_up, n_down = lax.rem(narrow + 1, narrow_size), lax.rem(narrow + narrow_size - 1, narrow_size)
    sides = ((w_up, narrow), (w_down, narrow), (wide, n_up), (wide, n_down))
    core, chip = lax.rem(wide, 2), wide // 2
    partner = (wide + 1 - 2 * core, narrow)
    wide_steps = sorted(range(1, chips), key=lambda d: -min(d, chips - d))
    narrow_steps = sorted(range(1, narrow_size), key=lambda d: -min(d, narrow_size - d))
    in_wide = [(2 * lax.rem(chip + d, chips) + core, narrow) for d in wide_steps]
    in_narrow = [(wide, lax.rem(narrow + d, narrow_size)) for d in narrow_steps]

    barrier = pltpu.get_barrier_semaphore()
    everyone = [sides[0], sides[1]] + in_narrow[::-1] + in_wide[::-1]
    for device in everyone:
        pl.semaphore_signal(barrier, inc=1, device_id=device, device_id_type=MESH)

    def remote(source, target, sent, received, device):
        return pltpu.make_async_remote_copy(
            src_ref=source, dst_ref=target, send_sem=sent, recv_sem=received,
            device_id=device, device_id_type=MESH,
        )

    kappa = iota((2 * COLS, COLS), 0)
    tail = kappa - COLS
    edge = jnp.where(tail < COLS // 2, tail % RANGE - RANGE, tail % RANGE + COLS)
    origin = jnp.where(kappa < COLS, kappa, edge) - iota((2 * COLS, COLS), 1)
    for t, step in enumerate(STEPS):
        shifter[:, COLS * t : COLS * (t + 1)] = ones_where(origin == step)

    spot_row = iota((COLS, 2 * COLS), 0)
    spot_band = spot_row % (COLS // 2) // RANGE
    spot_col = spot_row % RANGE + jnp.where(spot_row < COLS // 2, COLS - RANGE, 0)
    spot_lane = COLS * spot_band + spot_col - iota((COLS, 2 * COLS), 1)

    def transposed(source, field, plain, arrivals):
        count = VECS // len(arrivals)
        for part, arrival in enumerate(arrivals):
            arrival.wait()

            @pl.loop(count * part, count * (part + 1), unroll=8)
            def _(v):
                flat[pl.ds(pl.multiple_of(v * PITCH, 8), ROWS), :] = source[v].astype(F32)

        @pl.loop(0, ROWS, unroll=8)
        def _(row):
            groups = [flat[pl.ds(8 * g * PITCH + row, 8, stride=PITCH), :] for g in range(VECS // 8)]
            whole_row = jnp.concatenate(groups, axis=0)
            field[row + RANGE] = whole_row
            plain[row] = whole_row.astype(BF16)

    def edges(side, plain):
        row_send[side, 0] = plain[ROWS - RANGE : ROWS]
        row_send[side, 1] = plain[0:RANGE]
        sums = [jnp.zeros((COLS, COLS), F32) for _ in range(2)]
        for c in range(BANDS // 2):
            pick = ones_where(spot_lane == 2 * COLS * c)
            bands = [
                plain[RANGE * b : RANGE * (b + 1)].reshape(RANGE * VECS, COLS)
                for b in (2 * c, 2 * c + 1)
            ]
            both = jnp.concatenate(bands, axis=1)
            for n in range(2):
                sums[n] = sums[n] + lax.dot_general(
                    pick, both[COLS * n : COLS * (n + 1)], (((1,), (1,)), ((), ())),
                    preferred_element_type=F32,
                )
        picked = jnp.concatenate(sums, axis=1)
        col_send[side, 0] = picked[: COLS // 2].astype(BF16)
        col_send[side, 1] = picked[COLS // 2 :].astype(BF16)

    def copies(slot, row_pair, col_pair):
        made = []
        for way in range(4):
            (source, target), part = (row_pair, way) if way < 2 else (col_pair, way - 2)
            made.append(
                remote(
                    source.at[part], target.at[part], send_sem.at[slot, way], recv_sem.at[slot, way],
                    sides[way],
                )
            )
        return made

    def landed_rows(side, field, moves):
        for move in moves:
            move.wait_recv()
        field[0:RANGE] = row_recv[side, 0].astype(F32)
        field[ROWS + RANGE : ROWS + 2 * RANGE] = row_recv[side, 1].astype(F32)

    def landed_cols(side, packed, moves):
        for move in moves:
            move.wait_recv()
        strips = jnp.concatenate([col_recv[side, way].astype(F32) for way in range(2)], axis=0)
        packed[...] = jnp.transpose(strips).astype(BF16).reshape(RANGE, VECS, COLS)

    product[...] = jnp.zeros_like(product)
    back[1] = jnp.zeros_like(back[1])

    transposed(right_ref, field_r, plain_r, loads[:4])
    edges(0, plain_r)
    pl.semaphore_wait(barrier, len(everyone))
    moves_r = copies(0, (row_send.at[0], row_recv.at[0]), (col_send.at[0], col_recv.at[0]))
    for move in moves_r:
        move.start()

    transposed(left_ref, field_l, plain_l, loads[4:5])
    edges(1, plain_l)
    moves_l = copies(1, (row_send.at[1], row_recv.at[1]), (col_send.at[1], col_recv.at[1]))
    for move in moves_l:
        move.start()

    loads[5].wait()
    loads[6].wait()

    def coefficient(op, tap):
        return hop_ref[op, tap % RANGE] * (1.0 if tap < RANGE else -1.0)

    def sign_of(op, tap):
        return (2 * bits_ref[op, tap] - 1).astype(F32)

    small = iota((ROWS, COLS), 1)
    for half, op in enumerate((0, 2)):
        for tap in range(2 * RANGE):
            sign = sign_of(op, tap)
            weight[8 * op + tap, 8 : 8 + ROWS, :] = coefficient(op, tap) * sign
            way, at = (0, ROWS - RANGE) if tap < RANGE else (1, 0)
            spot = (4 * half + tap % RANGE) * RANGE
            sr_stage[way, spot : spot + RANGE, :] = sign[at : at + RANGE]
    for way in range(2):
        sr_send[way] = sr_stage[way].astype(BF16)
    for way in range(2):
        held = jnp.zeros((ROWS, COLS), F32)
        for half, op in enumerate((1, 3)):
            for k in range(RANGE):
                tap = RANGE * way + k
                sign = sign_of(op, tap)
                weight[8 * op + tap, 8 : 8 + ROWS, :] = coefficient(op, tap) * sign
                at = COLS // 2 * way + RANGE * (4 * half + k)
                moved = pltpu.roll(sign, at + RANGE if way == 0 else at, 1) if at or way == 0 else sign
                held = jnp.where(small // RANGE == at // RANGE, moved, held)
        sc_send[way] = held.astype(BF16)
    moves_s = copies(2, (sr_send, sr_recv), (sc_send, sc_recv))
    for move in moves_s:
        move.start()

    def along_rows(field, row, adjoint):
        sums = [None, None]
        for tap in range(2 * RANGE):
            step = -STEPS[tap] if adjoint else STEPS[tap]
            x = field[RANGE + row + step]
            for half, op in enumerate((0, 2)):
                at = 8 + row + (step if adjoint else 0)
                term = weight[8 * op + tap, pl.ds(at, 1), :] * x
                sums[half] = term if sums[half] is None else sums[half] + term
        return sums

    wide_lane = iota((VECS, COLS), 1) % (COLS // 2) // RANGE

    def shift_cols(plain, packed, band, slot):
        inside = wide_lane == band
        rows = []
        for j in range(RANGE):
            strip = packed[j]
            rows.append(
                jnp.concatenate([plain[RANGE * band + j], jnp.where(inside, strip, jnp.zeros_like(strip))], axis=1)
            )
        lhs = jnp.concatenate(rows, axis=0)
        for t in range(4):
            at = slice(2 * COLS * t, 2 * COLS * (t + 1))
            slid[slot, :, at] = jnp.dot(lhs, shifter[:, at], preferred_element_type=F32)

    def along_cols(slot, j, row, adjoint):
        sums = [None, None]
        for t in range(2 * RANGE):
            tap = (t + RANGE) % (2 * RANGE) if adjoint else t
            x = slid[slot, VECS * j : VECS * (j + 1), COLS * t : COLS * (t + 1)]
            for half, op in enumerate((1, 3)):
                if adjoint:
                    w = weight_adj[8 * half + tap, pl.ds(row, 1), :]
                else:
                    w = weight[8 * op + tap, pl.ds(8 + row, 1), :]
                term = w * x
                sums[half] = term if sums[half] is None else sums[half] + term
        return sums

    def applied(field, band, slot, adjoint, store):
        for j in range(RANGE):
            row = RANGE * band + j
            even = along_rows(field, row, adjoint)
            odd = along_cols(slot, j, row, adjoint)
            for op in range(OPS):
                value = (odd if op % 2 else even)[op // 2]
                store(slice(VECS * op, VECS * (op + 1)), slice(COLS * j, COLS * (j + 1)), value.astype(BF16))

    def row_ops(band):
        for j in range(RANGE):
            sums = along_rows(field_r, RANGE * band + j, False)
            for half, op in enumerate((0, 2)):
                first[band, VECS * op : VECS * (op + 1), COLS * j : COLS * (j + 1)] = sums[half].astype(BF16)

    def col_ops(band, slot):
        for j in range(RANGE):
            sums = along_cols(slot, j, RANGE * band + j, False)
            for half, op in enumerate((1, 3)):
                first[band, VECS * op : VECS * (op + 1), COLS * j : COLS * (j + 1)] = sums[half].astype(BF16)

    @pl.loop(1, BANDS - 1)
    def _(band):
        row_ops(band)

    landed_rows(0, field_r, moves_r[:2])
    for band in (0, BANDS - 1):
        row_ops(band)
    landed_cols(0, packed_r, moves_r[2:])
    shift_cols(plain_r, packed_r, 0, 0)

    @pl.loop(0, BANDS // 2)
    def _(couple):
        for slot in range(2):
            band = 2 * couple + slot
            col_ops(band, slot)
            shift_cols(plain_r, packed_r, jnp.minimum(band + 1, BANDS - 1), 1 - slot)

    for move in moves_s:
        move.wait_recv()
    landed_rows(1, field_l, moves_l[:2])
    landed_cols(1, packed_l, moves_l[2:])

    for way in range(2):
        sr_stage[way] = sr_recv[way].astype(F32)
    for half, op in enumerate((0, 2)):
        for tap in range(2 * RANGE):
            way, at = (0, 8 - RANGE) if tap < RANGE else (1, 8 + ROWS)
            spot = (4 * half + tap % RANGE) * RANGE
            weight[8 * op + tap, at : at + RANGE, :] = coefficient(op, tap) * sr_stage[way, spot : spot + RANGE, :]
    strips = sc_recv[0].astype(F32) + sc_recv[1].astype(F32)
    for tap in range(2 * RANGE):
        lhs = []
        for half, op in enumerate((1, 3)):
            spot = 4 * half + tap % RANGE
            inside = small % (COLS // 2) // RANGE == spot
            lhs.append(jnp.concatenate([sign_of(op, tap), jnp.where(inside, strips, 0.0)], axis=1))
        t = (tap + RANGE) % (2 * RANGE)
        moved = jnp.dot(
            jnp.concatenate(lhs, axis=0).astype(BF16), shifter[:, COLS * t : COLS * (t + 1)],
            preferred_element_type=F32,
        )
        for half, op in enumerate((1, 3)):
            weight_adj[8 * half + tap] = coefficient(op, tap) * moved[ROWS * half : ROWS * (half + 1)]

    def gram(band, slot):
        part = lax.dot_general(back[slot], first[band], (((1,), (1,)), ((), ())), preferred_element_type=F32)
        for h in range(2):
            product[h] += part[:, COLS * h : COLS * (h + 1)]

    shift_cols(plain_l, packed_l, 0, 0)

    @pl.loop(0, BANDS // 2)
    def _(couple):
        for slot in range(2):
            band = 2 * couple + slot

            def store(vecs, cols, value):
                back[slot, vecs, cols] = value

            applied(field_l, band, slot, True, store)
            shift_cols(plain_l, packed_l, jnp.minimum(band + 1, BANDS - 1), 1 - slot)
            gram(jnp.maximum(band - 1, 0), 1 - slot)

    gram(BANDS - 1, 1)

    def collect(side):
        @pl.loop(0, chips, unroll=4)
        def _(place):
            for h in range(2):
                for i in range(2):
                    parts[side, place, 4 * i : 4 * i + 4, COLS * h : COLS * (h + 1)] = product[
                        h, pl.ds(4 * place + 2 * side + i, 4, stride=VECS), :
                    ]

    collect(1 - core)
    swap = remote(parts.at[1 - core], arrived_core, core_send.at[0], core_recv.at[0], partner)
    swap.start()
    collect(core)
    swap.wait()
    own[...] = parts[core] + arrived_core[...]

    moves = []
    for d, device in enumerate(in_wide):
        target = lax.rem(chip + wide_steps[d], chips)
        moves.append(remote(own.at[target], arrived_wide.at[d], wide_send.at[d], wide_recv.at[d], device))
    for move in moves:
        move.start()
    for move in moves:
        move.wait_recv()
    total = own[chip]
    for d in range(chips - 1):
        total = total + arrived_wide[d]
    whole[...] = total

    sent = moves_r + moves_l + moves_s + moves
    moves = []
    for d, device in enumerate(in_narrow):
        moves.append(remote(whole, arrived_narrow.at[d], narrow_send.at[d], narrow_recv.at[d], device))
    for move in moves:
        move.start()
    for move in sent:
        move.wait_send()
    for move in moves:
        move.wait_recv()
    total = whole[...]
    for d in range(narrow_size - 1):
        total = total + arrived_narrow[d]
    for b in range(OPS):
        turn = lax.rem(2 * COLS - VECS * (b % 2) - 8 * narrow, COLS)
        mine = pltpu.roll(total[:, COLS * (b // 2) : COLS * (b // 2 + 1)], turn, 1)
        for i in range(2):
            staged[i, pl.ds(b, OPS, stride=OPS), :] = mine[OPS * i : OPS * (i + 1)]
    for i in range(2):
        out_ref[i] = jnp.transpose(staged[i])[: VECS // narrow_size]
    for move in moves:
        move.wait_send()


def on_device(left, right, bond_signs, hop):
    wide_size = lax.axis_size("wide")
    narrow_size = lax.axis_size("narrow")
    chips = wide_size // 2
    scale = 1.0 / math.sqrt(ROWS * COLS * wide_size * narrow_size)
    hbm = pl.BlockSpec(memory_space=pl.ANY)
    dma = pltpu.SemaphoreType.DMA
    block = (8, OPS * VECS)
    spread = pl.pallas_call(
        functools.partial(moments_kernel, chips),
        out_shape=jax.ShapeDtypeStruct((2, VECS // narrow_size, OPS * OPS), F32),
        in_specs=[hbm] * 4,
        out_specs=pl.BlockSpec(memory_space=pltpu.VMEM),
        scratch_shapes=[
            pltpu.VMEM((VECS, ROWS, COLS), BF16),
            pltpu.VMEM((VECS, ROWS, COLS), BF16),
            pltpu.VMEM((OPS, 2 * RANGE, ROWS, COLS), jnp.int32),
            pltpu.SMEM((OPS, RANGE), F32),
            pltpu.VMEM((VECS * PITCH, COLS), F32),
            pltpu.VMEM((ROWS + 2 * RANGE, VECS, COLS), F32),
            pltpu.VMEM((ROWS + 2 * RANGE, VECS, COLS), F32),
            pltpu.VMEM((ROWS, VECS, COLS), BF16),
            pltpu.VMEM((ROWS, VECS, COLS), BF16),
            pltpu.VMEM((8 * OPS, ROWS + 16, COLS), F32),
            pltpu.VMEM((16, ROWS, COLS), F32),
            pltpu.VMEM((2 * COLS, 8 * COLS), BF16),
            pltpu.VMEM((RANGE, VECS, COLS), BF16),
            pltpu.VMEM((RANGE, VECS, COLS), BF16),
            pltpu.VMEM((2, RANGE * VECS, 8 * COLS), F32),
            pltpu.VMEM((BANDS, OPS * VECS, RANGE * COLS), BF16),
            pltpu.VMEM((2, OPS * VECS, RANGE * COLS), BF16),
            pltpu.VMEM((2, OPS * VECS, COLS), F32),
            pltpu.VMEM((2, 2, RANGE, VECS, COLS), BF16),
            pltpu.VMEM((2, 2, RANGE, VECS, COLS), BF16),
            pltpu.VMEM((2, 2, COLS // 2, 2 * COLS), BF16),
            pltpu.VMEM((2, 2, COLS // 2, 2 * COLS), BF16),
            pltpu.VMEM((2, 8 * RANGE, COLS), F32),
            pltpu.VMEM((2, 8 * RANGE, COLS), BF16),
            pltpu.VMEM((2, 8 * RANGE, COLS), BF16),
            pltpu.VMEM((2, ROWS, COLS), BF16),
            pltpu.VMEM((2, ROWS, COLS), BF16),
            pltpu.VMEM((2, chips) + block, F32),
            pltpu.VMEM((chips,) + block, F32),
            pltpu.VMEM((chips,) + block, F32),
            pltpu.VMEM((chips - 1,) + block, F32),
            pltpu.VMEM(block, F32),
            pltpu.VMEM((narrow_size - 1,) + block, F32),
            pltpu.VMEM((2, OPS * OPS, COLS), F32),
            dma((7,)),
            dma((3, 4)),
            dma((3, 4)),
            dma((1,)),
            dma((1,)),
            dma((chips - 1,)),
            dma((chips - 1,)),
            dma((narrow_size - 1,)),
            dma((narrow_size - 1,)),
        ],
        compiler_params=pltpu.CompilerParams(
            collective_id=0, has_side_effects=True, vmem_limit_bytes=60 << 20
        ),
        name="moments",
    )(left, right, bond_signs, hop)
    return spread.transpose(2, 0, 1) * F32(scale)


def solution(mesh):
    in_specs = (
        P(None, "wide", "narrow"),
        P(None, "wide", "narrow"),
        P(None, None, "wide", "narrow"),
        P(),
    )
    return jax.shard_map(
        on_device, mesh=mesh, in_specs=in_specs, out_specs=P(None, "wide", "narrow"), check_vma=False
    )
```
